32 devices in a mesh: dom: 32 (over z, y, x, core).
Axes of the slice: x: 2, y: 2, z: 4, core: 2. Of those that a mesh axis runs over, the one named last changes fastest.
Arguments:
- right_side: float32 [1024, 16, 128], P('dom')
- band_blocks: float32 [1024, 5, 128, 128], P('dom'), as said below
- link_blocks: float32 [32, 6, 4, 128, 128], P('dom'), as said below
- link_rows: int32 [32, 6, 4], P('dom'), may hold values from 0 to 32, as said below
Outputs:
- solution: float32 [1024, 16, 128], P('dom')
- residual: float32 [1024, 16, 128], P('dom')
The draws below stay inside these ranges and needn't reach their ends.
Inputs may be any that keep to these rules, and one draw needn't show every extreme that they name: `link_rows`: entries are a row of device d (0 to 31) or 32 for an unused slot. Slot s of interface j of device d is paired with slot s of interface j xor 1 of the device it faces, and is used exactly when that one is. Each interface uses its first 1 to 4 slots and no row twice; in every draw some interface uses all 4. link_blocks[d, j, s] is the transpose of link_blocks[e, j xor 1, s] for the device e that interface j of d faces; blocks of unused slots are zero. band_blocks[g, 2 + m] is the transpose of band_blocks[g + m, 2 - m]; blocks whose column falls outside the device are zero. A is symmetric with a positive diagonal that exceeds the sum of magnitudes of the rest of its row.
All inputs are finite; a program needn't handle non-finite values.
Results may differ from the reference program's by a relative error of at most 0.0003.
Values sent between devices are 32-bit elements; how exact they have to be, the bound alone decides.
No kernel may reach another device: no remote copies, remote signals or barrier semaphores. Data moves between devices by JAX's collectives and lax.ppermute only.
A program may use at most 64 MiB of HBM per device.

```python
import jax
import jax.numpy as jnp
from jax import lax

BS = 128
S = 16
R_DEV = 32
ITERS = 3
H = 4
NB = 1024
N_DOM = 32


def facing_offsets_drawn(dev_count):
    return (1, -1, dev_count // 16, -(dev_count // 16), dev_count // 4, -(dev_count // 4))


def rough_block(key, shape):
    weight = 1.0 / (7.0 * BS)
    spread = jax.random.uniform(key, shape, jnp.float32, 0.5, 1.5)
    return -weight * spread


def build_matrix(key):
    dev_count = N_DOM
    block_rows = R_DEV
    links = H
    offset_list = facing_offsets_drawn(dev_count)
    keys = jax.random.split(jax.random.fold_in(key, 11), 7)
    counts = jax.random.randint(keys[0], (dev_count, 3), 1, links + 1)
    fullest = jax.random.randint(keys[1], (3,), 0, dev_count)
    counts = counts.at[fullest, jnp.arange(3)].set(links)
    orders = jax.vmap(lambda sub: jax.random.permutation(sub, block_rows))(jax.random.split(keys[2], dev_count))
    slots = jnp.arange(links)
    used_list = []
    rows_list = []
    for facing in range(6):
        pair = facing // 2
        if facing % 2 == 0:
            owned = counts[:, pair]
        else:
            owned = jnp.roll(counts[:, pair], offset_list[facing - 1])
        used = slots[None, :] < owned[:, None]
        picked = orders[:, (facing * links + slots) % block_rows]
        used_list.append(used)
        rows_list.append(jnp.where(used, picked, block_rows).astype(jnp.int32))
    link_rows = jnp.stack(rows_list, axis=1)
    raw = rough_block(keys[3], (dev_count, 3, links, BS, BS))
    blocks_list = []
    for facing in range(6):
        pair = facing // 2
        kept = raw[:, pair] * used_list[2 * pair][:, :, None, None].astype(jnp.float32)
        if facing % 2 == 0:
            blocks_list.append(kept)
        else:
            blocks_list.append(jnp.roll(jnp.swapaxes(kept, -1, -2), offset_list[2 * pair], axis=0))
    link_blocks = jnp.stack(blocks_list, axis=1)
    upper = rough_block(keys[4], (dev_count, block_rows, 2, BS, BS))
    places = jnp.arange(block_rows)[:, None] + jnp.arange(1, 3)[None, :]
    upper = upper * (places < block_rows).astype(jnp.float32)[None, :, :, None, None]
    lower_one = jnp.swapaxes(jnp.roll(upper[:, :, 0], 1, axis=1), -1, -2)
    lower_two = jnp.swapaxes(jnp.roll(upper[:, :, 1], 2, axis=1), -1, -2)
    inner = rough_block(keys[5], (dev_count, block_rows, BS, BS))
    inner = 0.5 * (inner + jnp.swapaxes(inner, -1, -2))
    identity = jnp.eye(BS, dtype=jnp.float32)
    inner = inner * (1.0 - identity)
    row_abs = jnp.sum(jnp.abs(inner), axis=-1)
    row_abs = row_abs + jnp.sum(jnp.abs(upper), axis=(2, 4))
    row_abs = row_abs + jnp.sum(jnp.abs(lower_one), axis=-1) + jnp.sum(jnp.abs(lower_two), axis=-1)
    picks = (link_rows[:, :, :, None] == jnp.arange(block_rows)[None, None, None, :]).astype(jnp.float32)
    row_abs = row_abs + jnp.einsum('cjhr,cjhi->cri', picks, jnp.sum(jnp.abs(link_blocks), axis=-1))
    low, high = (0.05, 4.0)
    margin = jnp.exp(jax.random.uniform(keys[6], (dev_count, block_rows, BS), jnp.float32, jnp.log(low), jnp.log(high)))
    diagonal = inner + identity * (row_abs + margin)[..., :, None]
    band = jnp.stack([lower_two, lower_one, diagonal, upper[:, :, 0], upper[:, :, 1]], axis=2)
    return (link_rows, band.reshape(dev_count * block_rows, 5, BS, BS), link_blocks)


def draw_link_rows(key, part):
    return build_matrix(key)[0]


def draw_band_blocks(key, part):
    return build_matrix(key)[1]


def draw_link_blocks(key, part):
    return build_matrix(key)[2]


def draw_right_side(key, part):
    noise = jax.random.normal(jax.random.fold_in(key, 3), (NB, S, BS), jnp.float32)
    owner = (jnp.arange(NB) // R_DEV).astype(jnp.float32)
    rising = (1.0 + 2.0 * owner / (N_DOM - 1))[:, None, None]
    return noise * rising


def setup_inputs(seed: int = 0) -> dict:
    seeds = jax.random.split(jax.random.key(seed), 5)
    return {
        "right_side": draw_right_side(jax.random.fold_in(seeds[4], 71), 0),
        "band_blocks": draw_band_blocks(jax.random.fold_in(seeds[4], 71), 0),
        "link_blocks": draw_link_blocks(jax.random.fold_in(seeds[4], 71), 0),
        "link_rows": draw_link_rows(jax.random.fold_in(seeds[4], 71), 0),
    }


HIGHEST = lax.Precision.HIGHEST

def facing_offsets(dev_count):
    return (1, -1, dev_count // 16, -(dev_count // 16), dev_count // 4, -(dev_count // 4))

def apply_matrix(field, band_blocks, link_blocks, link_rows):
    dev_count = N_DOM
    block_rows = R_DEV
    shards = field.reshape(dev_count, block_rows, S, BS)
    padded = jnp.pad(shards, ((0, 0), (2, 2), (0, 0), (0, 0)))
    banded = band_blocks.reshape(dev_count, block_rows, 5, BS, BS)
    total = jnp.zeros_like(shards)
    for band_slot in range(5):
        total = total + jnp.einsum('nrsj,nrij->nrsi', padded[:, band_slot:band_slot + block_rows], banded[:, :, band_slot], precision=HIGHEST)
    extended = jnp.concatenate([shards, jnp.zeros((dev_count, 1, S, BS), field.dtype)], axis=1)
    devices = jnp.arange(dev_count, dtype=jnp.int32)
    offset_list = facing_offsets(dev_count)
    for facing in range(6):
        partner = ((devices + offset_list[facing]) % dev_count).astype(jnp.int32)
        far_rows = link_rows[partner, facing ^ 1]
        arrived = extended[partner[:, None], far_rows]
        contrib = jnp.einsum('nhsj,nhij->nhsi', arrived, link_blocks[:, facing], precision=HIGHEST)
        landing = jnp.zeros((dev_count, block_rows + 1, S, BS), field.dtype)
        landing = landing.at[devices[:, None], link_rows[:, facing]].add(contrib)
        total = total + landing[:, :block_rows]
    return total.reshape(NB, S, BS)

def gram_matrix(left, right):
    return jnp.einsum('nsi,nti->st', left, right, precision=HIGHEST)

def mix_columns(field, coeffs):
    return jnp.einsum('nsi,st->nti', field, coeffs, precision=HIGHEST)

def solve_gram(matrix, target):
    symmetric = 0.5 * (matrix + matrix.T)
    factor = jnp.linalg.cholesky(symmetric)
    return jax.scipy.linalg.cho_solve((factor, True), target)

def reference(right_side, band_blocks, link_blocks, link_rows):
    solution = jnp.zeros_like(right_side)
    residual = right_side
    direction = right_side
    squares = gram_matrix(residual, residual)
    for iteration in range(ITERS):
        image = apply_matrix(direction, band_blocks, link_blocks, link_rows)
        alpha = solve_gram(gram_matrix(direction, image), squares)
        solution = solution + mix_columns(direction, alpha)
        residual = residual - mix_columns(image, alpha)
        if iteration + 1 < ITERS:
            fresh = gram_matrix(residual, residual)
            beta = solve_gram(squares, fresh)
            direction = residual + mix_columns(direction, beta)
            squares = fresh
    return (solution, residual)
```

```python
import functools

import jax
import jax.numpy as jnp
from jax import lax
from jax.experimental import pallas as pl
from jax.experimental.pallas import tpu as pltpu
from jax.sharding import PartitionSpec as P


ITERS = 3
LEVELS = ITERS + 1
PIECES = 3
F32 = jnp.float32
BF16 = jnp.bfloat16
MIB = 1 << 20

MATCHINGS = ((0, 1), (1, 1), (2, 1), (2, 0), (1, 0), (0, 0))


def offsets(dev_count):
    return (1, dev_count // 16, dev_count // 4)


def matching_pairs(dev_count, pair, phase):
    off = offsets(dev_count)[pair]
    return [
        (i, (i + off) % dev_count if (i // off + phase) % 2 == 0 else (i - off) % dev_count)
        for i in range(dev_count)
    ]


def matching_face(dev_count, pair, phase):
    me = lax.axis_index("dom")
    return 2 * pair + lax.rem(me // offsets(dev_count)[pair] + phase, 2)


def pieces_of(value):
    high = value.astype(BF16)
    rest = value - high.astype(F32)
    mid = rest.astype(BF16)
    low = (rest - mid.astype(F32)).astype(BF16)
    return high, mid, low


def vmem(count):
    return [pl.BlockSpec(memory_space=pltpu.VMEM)] * count


def smem():
    return pl.BlockSpec(memory_space=pltpu.SMEM)


def params(mib):
    return pltpu.CompilerParams(vmem_limit_bytes=mib * MIB)


def send_rows(dev_count, rows_ref, field_ref, out_refs):
    block_rows = field_ref.shape[0]
    for (pair, phase), out_ref in zip(MATCHINGS, out_refs):
        face = matching_face(dev_count, pair, phase)
        for slot in range(rows_ref.shape[2]):
            row = jnp.minimum(rows_ref[0, face, slot], block_rows - 1)
            out_ref[slot] = field_ref[row]


def split_field(field_ref, split_ref, pad):
    block_rows, width, size = field_ref.shape
    zero = jnp.zeros((split_ref.shape[0], pad * size), BF16)
    split_ref[:, : pad * size] = zero
    split_ref[:, (pad + block_rows) * size :] = zero
    for row in range(block_rows):
        cols = slice((pad + row) * size, (pad + row + 1) * size)
        for piece, value in enumerate(pieces_of(field_ref[row])):
            split_ref[piece * width : (piece + 1) * width, cols] = value


def first_send_kernel(dev_count, rows_ref, field_ref, *out_refs):
    send_rows(dev_count, rows_ref, field_ref, out_refs)


def prepare_kernel(half, field_ref, band_ref, link_ref, weights_ref, links_ref, split_ref, held, sems, link_held, link_sem):
    block_rows, band, size, _ = band_ref.shape
    pairs = block_rows // 2
    span = band + 1
    slots = held.shape[0]

    def fetch(row, slot):
        return pltpu.make_async_copy(band_ref.at[row], held.at[slot], sems.at[slot])

    link_copy = pltpu.make_async_copy(link_ref.at[0], link_held, link_sem)
    for row in range(slots):
        fetch(row, row).start()
    link_copy.start()
    split_field(field_ref, split_ref, half)
    zero = jnp.zeros((size, size), BF16)

    def clear(pair, carry):
        for copy in range(2):
            weights_ref[pair, copy * span, :, size:] = zero
            weights_ref[pair, copy * span + span - 1, :, :size] = zero
        return carry

    lax.fori_loop(0, pairs + 2, clear, 0)
    wide = jnp.zeros((size, 2 * size), BF16)
    for copy in range(2):
        for place in range(half):
            weights_ref[1, copy * span + place] = wide
            weights_ref[pairs, copy * span + span - 1 - place] = wide

    def convert(step, carry):
        for even in range(slots):
            row = slots * step + even
            fetch(row, even).wait()
            base = slots // 2 * step + even // 2
            for k in range(band):
                shift = (even % 2 + k - half) // 2
                col = (even % 2 + k - half) % 2
                place = even % 2 + half - 2 * shift
                block = held[even, k]
                high = block.astype(BF16)
                low = (block - high.astype(F32)).astype(BF16)
                cols = slice(col * size, (col + 1) * size)
                weights_ref[base + shift + 1, place, :, cols] = high
                weights_ref[base + shift + 1, span + place, :, cols] = low

            @pl.when(row + slots < block_rows)
            def _():
                fetch(row + slots, even).start()

        return carry

    lax.fori_loop(0, block_rows // slots, convert, 0)
    link_copy.wait()
    faces, count = link_held.shape[0], link_held.shape[1]

    def convert_links(face, carry):
        for slot in range(count):
            block = link_held[face, slot].T
            high = block.astype(BF16)
            low = (block - high.astype(F32)).astype(BF16)
            cols = slice(slot % 2 * size, (slot % 2 + 1) * size)
            links_ref[face, slot // 2, :size, cols] = high
            links_ref[face, slot // 2, size:, cols] = low
        return carry

    lax.fori_loop(0, faces, convert_links, 0)


def fold(value, width):
    total = value[(PIECES - 1) * width : PIECES * width]
    for piece in range(PIECES - 2, -1, -1):
        total = total + value[piece * width : (piece + 1) * width]
    return total


def band_kernel(weights_ref, split_ref, out_ref):
    block_rows, width, size = out_ref.shape
    pairs = block_rows // 2
    depth = weights_ref.shape[1] * size
    span = depth // 2

    def pair_product(pair, carry):
        start = pl.multiple_of(pair * 2 * size, 2 * size)
        rows = split_ref[:, pl.ds(start, span)]
        both = jnp.concatenate([rows, rows], axis=1)
        weights = weights_ref[pair + 1].reshape(depth, 2 * size)
        total = fold(jnp.dot(both, weights, preferred_element_type=F32), width)
        out_ref[2 * pair] = total[:, :size]
        out_ref[2 * pair + 1] = total[:, size:]
        return carry

    lax.fori_loop(0, pairs, pair_product, 0, unroll=4)


def add_links(dev_count, rows_ref, base_ref, links_ref, far_refs, field_ref):
    block_rows, width, size = base_ref.shape
    field_ref[...] = base_ref[...]
    for (pair, phase), far_ref in zip(MATCHINGS, far_refs):
        face = matching_face(dev_count, pair, phase)
        for two in range(far_ref.shape[0] // 2):
            stacked = []
            for slot in (2 * two, 2 * two + 1):
                stacked.extend(pieces_of(far_ref[slot]))
            rows = jnp.concatenate(stacked, axis=0)
            both = jnp.concatenate([rows, rows], axis=1)
            product = jnp.dot(both, links_ref[face, two], preferred_element_type=F32)
            for k in range(2):
                part = product[k * PIECES * width : (k + 1) * PIECES * width, k * size : (k + 1) * size]
                row = jnp.minimum(rows_ref[0, face, 2 * two + k], block_rows - 1)
                field_ref[row] = field_ref[row] + fold(part, width)


def link_kernel(dev_count, pad, rows_ref, base_ref, links_ref, *refs):
    count = len(MATCHINGS)
    far_refs, split_ref, out_refs, field_ref = refs[:count], refs[count], refs[count + 1 : -1], refs[-1]
    add_links(dev_count, rows_ref, base_ref, links_ref, far_refs, field_ref)
    send_rows(dev_count, rows_ref, field_ref, out_refs)
    split_field(field_ref, split_ref, pad)


def gram_rows(left, split_refs, cols):
    width = split_refs[0].shape[0] // PIECES
    right = [ref[piece * width : (piece + 1) * width, cols] for piece in range(PIECES) for ref in split_refs]
    fill = [jnp.zeros_like(right[0])] * (2 * 128 // width - len(right))
    return lax.dot_general(
        left, jnp.concatenate(right + fill, axis=0), (((1,), (1,)), ((), ())), preferred_element_type=F32
    )


def fold_lanes(value):
    first = value[:, :128]
    return value[:, 128:] + (first + pltpu.roll(first, 64, 1))


def gram_kernel(pad, split0, split1, split2, out_ref, total):
    rows, lanes = split0.shape
    width = rows // PIECES
    refs = (split0, split1, split2, split2)
    inner = lanes - 2 * pad * 128
    chunk = inner // 8
    total[...] = jnp.zeros_like(total)

    def body(step, carry):
        cols = pl.ds(pl.multiple_of(pad * 128 + step * chunk, 128), chunk)
        left = jnp.concatenate([ref[:, cols] for ref in refs[:3]], axis=0)
        total[...] += gram_rows(left, refs, cols)
        return carry

    lax.fori_loop(0, 8, body, 0)
    z = [fold_lanes(fold(total[rows * k : rows * (k + 1)], width)) for k in range(3)]
    lane = lax.broadcasted_iota(jnp.int32, z[0].shape, 1)
    out_ref[...] = jnp.where(
        lane < 2 * width,
        z[0],
        jnp.where(lane < 4 * width, pltpu.roll(z[1], width, 1), pltpu.roll(z[2], 2 * width, 1)),
    )


def last_link_kernel(dev_count, pad, rows_ref, base_ref, links_ref, split2, moments_ref, *refs):
    count = len(MATCHINGS)
    far_refs, split_ref, out_ref, field_ref = refs[:count], refs[count], refs[count + 1], refs[-1]
    add_links(dev_count, rows_ref, base_ref, links_ref, far_refs, field_ref)
    split_field(field_ref, split_ref, pad)
    rows, lanes = split2.shape
    width = rows // PIECES
    cols = slice(pad * 128, lanes - pad * 128)
    z = fold_lanes(fold(gram_rows(split2[:, cols], (split2, split2, split2, split_ref), cols), width))
    lane = lax.broadcasted_iota(jnp.int32, z.shape, 1)
    mine = jnp.where(lane < 5 * width, moments_ref[...], pltpu.roll(z, 2 * width, 1))
    mine = jnp.where(lane < 6 * width, mine, 0.0)
    for peer in range(out_ref.shape[0]):
        out_ref[peer] = mine


def finish_kernel(pad, gathered_ref, split0, split1, split2, split3, solution_ref, residual_ref):
    peers, width, lanes = gathered_ref.shape
    block_rows = solution_ref.shape[0]
    moments = gathered_ref[0]
    for peer in range(1, peers):
        moments = moments + gathered_ref[peer]
    table = [pltpu.roll(moments, lanes - width * (k + 1), 1) for k in range(ITERS)] + [moments]
    table = jnp.concatenate(table, axis=0)
    lane = lax.broadcasted_iota(jnp.int32, (1, lanes), 1)
    for k in range(ITERS * width):
        row = table[k : k + 1, :]
        column = table[:, k : k + 1] * (1.0 / table[k : k + 1, k : k + 1])
        table = jnp.where(lane == k, column, table - column * row)
    coeffs = table[ITERS * width :]
    lane = lax.broadcasted_iota(jnp.int32, coeffs.shape, 1)
    unit = (lane == lax.broadcasted_iota(jnp.int32, coeffs.shape, 0)).astype(F32)
    for_solution = jnp.where(lane < ITERS * width, coeffs, 0.0)
    for_residual = jnp.where(lane < width, unit, jnp.where(lane < LEVELS * width, -pltpu.roll(coeffs, width, 1), 0.0))
    both = jnp.concatenate([for_solution, for_residual], axis=0)
    both = jnp.concatenate([both + pltpu.roll(both, 64, 1), both], axis=1)[:, : PIECES * LEVELS * width]
    left = jnp.concatenate(pieces_of(both), axis=0)
    refs = (split0, split1, split2, split3)
    step = 4

    def body(index, carry):
        cols = pl.ds(pl.multiple_of((pad + index * step) * 128, 128), step * 128)
        right = [ref[piece * width : (piece + 1) * width, cols] for piece in range(PIECES) for ref in refs]
        total = fold(jnp.dot(left, jnp.concatenate(right, axis=0), preferred_element_type=F32), 2 * width)
        for k in range(step):
            solution_ref[index * step + k] = total[:width, k * 128 : (k + 1) * 128]
            residual_ref[index * step + k] = total[width:, k * 128 : (k + 1) * 128]
        return carry

    lax.fori_loop(0, block_rows // step, body, 0, unroll=2)


def shards(right_side, band_blocks, link_blocks, link_rows):
    dev_count = lax.axis_size("dom")
    block_rows, width, size = right_side.shape
    band = band_blocks.shape[1]
    half = band // 2
    faces, slots = link_rows.shape[1:]
    pairs = block_rows // 2
    count = len(MATCHINGS)
    message = jax.ShapeDtypeStruct((slots, width, size), F32)
    split = jax.ShapeDtypeStruct((PIECES * width, (block_rows + 2 * half) * size), BF16)
    field = jax.ShapeDtypeStruct(right_side.shape, F32)

    def exchange(messages):
        got = []
        for index, (pair, phase) in enumerate(MATCHINGS):
            got.append(lax.ppermute(messages[index], "dom", matching_pairs(dev_count, pair, phase)))
        return got

    messages = pl.pallas_call(
        functools.partial(first_send_kernel, dev_count),
        out_shape=[message] * count,
        in_specs=[smem()] + vmem(1),
        out_specs=vmem(count),
        compiler_params=params(8),
        name="first_send",
    )(link_rows, right_side)
    far = exchange(messages)
    weights, links, split0 = pl.pallas_call(
        functools.partial(prepare_kernel, half),
        out_shape=[
            jax.ShapeDtypeStruct((pairs + 2, 2 * (band + 1), size, 2 * size), BF16),
            jax.ShapeDtypeStruct((faces, slots // 2, 2 * size, 2 * size), BF16),
            split,
        ],
        in_specs=vmem(1) + [pl.BlockSpec(memory_space=pl.ANY)] * 2,
        out_specs=vmem(3),
        scratch_shapes=[
            pltpu.VMEM((4, band, size, size), F32),
            pltpu.SemaphoreType.DMA((4,)),
            pltpu.VMEM((faces, slots, size, size), F32),
            pltpu.SemaphoreType.DMA,
        ],
        compiler_params=params(28),
        cost_estimate=pl.CostEstimate(flops=10**7, bytes_accessed=12 * 10**6, transcendentals=0),
        name="prepare",
    )(right_side, band_blocks, link_blocks)

    splits = [split0]
    for level in range(ITERS):
        base = pl.pallas_call(
            band_kernel,
            out_shape=field,
            in_specs=vmem(2),
            out_specs=vmem(1)[0],
            compiler_params=params(24),
            cost_estimate=pl.CostEstimate(flops=10**9, bytes_accessed=12 * 10**6, transcendentals=0),
            name="band",
        )(weights, splits[-1])
        if level + 1 < ITERS:
            outs = pl.pallas_call(
                functools.partial(link_kernel, dev_count, half),
                out_shape=[split] + [message] * count,
                in_specs=[smem()] + vmem(2 + count),
                out_specs=vmem(1 + count),
                scratch_shapes=[pltpu.VMEM(right_side.shape, F32)],
                compiler_params=params(12),
                name="link",
            )(link_rows, base, links, *far)
            splits.append(outs[0])
            far = exchange(outs[1:])
    moments = pl.pallas_call(
        functools.partial(gram_kernel, half),
        out_shape=jax.ShapeDtypeStruct((width, 128), F32),
        in_specs=vmem(ITERS),
        out_specs=vmem(1)[0],
        scratch_shapes=[pltpu.VMEM((ITERS * PIECES * width, 256), F32)],
        compiler_params=params(8),
        cost_estimate=pl.CostEstimate(flops=10**9, bytes_accessed=4 * 10**6, transcendentals=0),
        name="gram",
    )(*splits)
    split3, mine = pl.pallas_call(
        functools.partial(last_link_kernel, dev_count, half),
        out_shape=[split, jax.ShapeDtypeStruct((dev_count, width, 128), F32)],
        in_specs=[smem()] + vmem(4 + count),
        out_specs=vmem(2),
        scratch_shapes=[pltpu.VMEM(right_side.shape, F32)],
        compiler_params=params(12),
        name="last_link",
    )(link_rows, base, links, splits[-1], moments, *far)
    splits.append(split3)
    gathered = lax.all_to_all(mine, "dom", 0, 0)
    return pl.pallas_call(
        functools.partial(finish_kernel, half),
        out_shape=[field, field],
        in_specs=vmem(1 + LEVELS),
        out_specs=vmem(2),
        compiler_params=params(12),
        name="finish",
    )(gathered, *splits)


def solution(mesh):
    in_specs = (
        P("dom", None, None),
        P("dom", None, None, None),
        P("dom", None, None, None, None),
        P("dom", None, None),
    )
    out_specs = (P("dom", None, None), P("dom", None, None))
    return jax.shard_map(
        lambda *args: tuple(shards(*args)), mesh=mesh, in_specs=in_specs, out_specs=out_specs, check_vma=False
    )
```

```python
import functools

import jax
import jax.numpy as jnp
from jax import lax
from jax.experimental import pallas as pl
from jax.experimental.pallas import tpu as pltpu
from jax.sharding import PartitionSpec as P


ITERS = 3
LEVELS = ITERS + 1
PIECES = 3
F32 = jnp.float32
BF16 = jnp.bfloat16
MIB = 1 << 20

MATCHINGS = ((0, 1), (1, 1), (2, 1), (2, 0), (1, 0), (0, 0))


def offsets(dev_count):
    return (1, dev_count // 16, dev_count // 4)


def matching_pairs(dev_count, pair, phase):
    off = offsets(dev_count)[pair]
    return [
        (i, (i + off) % dev_count if (i // off + phase) % 2 == 0 else (i - off) % dev_count)
        for i in range(dev_count)
    ]


def matching_face(dev_count, pair, phase):
    me = lax.axis_index("dom")
    return 2 * pair + lax.rem(me // offsets(dev_count)[pair] + phase, 2)


def pieces_of(value):
    high = value.astype(BF16)
    rest = value - high.astype(F32)
    mid = rest.astype(BF16)
    low = (rest - mid.astype(F32)).astype(BF16)
    return high, mid, low


def vmem(count):
    return [pl.BlockSpec(memory_space=pltpu.VMEM)] * count


def smem():
    return pl.BlockSpec(memory_space=pltpu.SMEM)


def params(mib):
    return pltpu.CompilerParams(vmem_limit_bytes=mib * MIB)


def send_rows(dev_count, rows_ref, field_ref, out_refs):
    block_rows = field_ref.shape[0]
    for (pair, phase), out_ref in zip(MATCHINGS, out_refs):
        face = matching_face(dev_count, pair, phase)
        for slot in range(rows_ref.shape[1]):
            row = jnp.minimum(rows_ref[0, slot, face], block_rows - 1)
            out_ref[slot] = field_ref[row]


def split_field(field_ref, split_ref, pad):
    block_rows, width, size = field_ref.shape
    zero = jnp.zeros((split_ref.shape[0], pad * size), BF16)
    split_ref[:, : pad * size] = zero
    split_ref[:, (pad + block_rows) * size :] = zero
    for row in range(block_rows):
        cols = slice((pad + row) * size, (pad + row + 1) * size)
        for piece, value in enumerate(pieces_of(field_ref[row])):
            split_ref[piece * width : (piece + 1) * width, cols] = value


def first_send_kernel(dev_count, rows_ref, field_ref, *refs):
    out_refs, sems = refs[:-1], refs[-1]
    block_rows = field_ref.shape[0]
    copies = []
    for hop, ((pair, phase), out_ref) in enumerate(zip(MATCHINGS, out_refs)):
        face = matching_face(dev_count, pair, phase)
        for slot in range(rows_ref.shape[1]):
            row = jnp.minimum(rows_ref[0, slot, face], block_rows - 1)
            copies.append(pltpu.make_async_copy(field_ref.at[row], out_ref.at[slot], sems.at[hop, slot]))
            copies[-1].start()
    for copy in copies:
        copy.wait()


def fold(value, width):
    total = value[(PIECES - 1) * width : PIECES * width]
    for piece in range(PIECES - 2, -1, -1):
        total = total + value[piece * width : (piece + 1) * width]
    return total


def pair_product(weights_ref, split_ref, out_ref, pair):
    _, width, size = out_ref.shape
    depth = weights_ref.shape[1] * size
    start = pl.multiple_of(pair * 2 * size, 2 * size)
    rows = split_ref[:, pl.ds(start, depth // 2)]
    both = jnp.concatenate([rows, rows], axis=1)
    weights = weights_ref[pair + 1].reshape(depth, 2 * size)
    total = fold(jnp.dot(both, weights, preferred_element_type=F32), width)
    out_ref[2 * pair] = total[:, :size]
    out_ref[2 * pair + 1] = total[:, size:]


def band_kernel(weights_ref, split_ref, out_ref):
    def body(pair, carry):
        pair_product(weights_ref, split_ref, out_ref, pair)
        return carry

    lax.fori_loop(0, out_ref.shape[0] // 2, body, 0, unroll=4)


def prepare_kernel(
    half, field_hbm, band_hbm, link_hbm, weights_ref, links_ref, split_ref, out_ref, field_ref, band_ref, link_ref, sems
):
    block_rows, band, size, _ = band_ref.shape
    faces, count = link_ref.shape[:2]
    pairs = block_rows // 2
    span = band + 1
    copies = [pltpu.make_async_copy(field_hbm, field_ref, sems.at[pairs])]
    copies += [
        pltpu.make_async_copy(band_hbm.at[pl.ds(2 * pair, 2)], band_ref.at[pl.ds(2 * pair, 2)], sems.at[pair])
        for pair in range(pairs)
    ]
    copies.append(pltpu.make_async_copy(link_hbm.at[0], link_ref, sems.at[pairs + 1]))
    for copy in copies:
        copy.start()
    wide = jnp.zeros((size, 2 * size), BF16)
    for copy in range(2):
        for place in range(half):
            weights_ref[1, copy * span + place] = wide
            weights_ref[pairs, copy * span + span - 1 - place] = wide
        for pair in range(1, pairs + 1):
            weights_ref[pair, copy * span, :, size:] = wide[:, :size]
            weights_ref[pair, copy * span + span - 1, :, :size] = wide[:, :size]
    copies[0].wait()
    split_field(field_ref, split_ref, half)

    def convert(step, carry):
        here = pl.ds(2 * step, 2)
        pltpu.make_async_copy(band_hbm.at[here], band_ref.at[here], sems.at[step]).wait()
        for even in range(2):
            for k in range(band):
                shift = (even + k - half) // 2
                col = (even + k - half) % 2
                place = even + half - 2 * shift
                block = band_ref[2 * step + even, k]
                high = block.astype(BF16)
                low = (block - high.astype(F32)).astype(BF16)
                cols = slice(col * size, (col + 1) * size)
                weights_ref[step + shift + 1, place, :, cols] = high
                weights_ref[step + shift + 1, span + place, :, cols] = low
        pair_product(weights_ref, split_ref, out_ref, jnp.maximum(step - 1, 0))
        return carry

    lax.fori_loop(0, pairs, convert, 0)
    pair_product(weights_ref, split_ref, out_ref, pairs - 1)
    copies[-1].wait()

    def convert_links(face, carry):
        for slot in range(count):
            block = link_ref[face, slot].T
            high = block.astype(BF16)
            low = (block - high.astype(F32)).astype(BF16)
            cols = slice(slot % 2 * size, (slot % 2 + 1) * size)
            links_ref[face, slot // 2, :size, cols] = high
            links_ref[face, slot // 2, size:, cols] = low
        return carry

    lax.fori_loop(0, faces, convert_links, 0)


def add_links(dev_count, rows_ref, base_ref, links_ref, far_refs, field_ref):
    block_rows, width, size = base_ref.shape
    field_ref[...] = base_ref[...]
    for (pair, phase), far_ref in zip(MATCHINGS, far_refs):
        face = matching_face(dev_count, pair, phase)
        for two in range(far_ref.shape[0] // 2):
            stacked = []
            for slot in (2 * two, 2 * two + 1):
                stacked.extend(pieces_of(far_ref[slot]))
            rows = jnp.concatenate(stacked, axis=0)
            both = jnp.concatenate([rows, rows], axis=1)
            product = jnp.dot(both, links_ref[face, two], preferred_element_type=F32)
            for k in range(2):
                part = product[k * PIECES * width : (k + 1) * PIECES * width, k * size : (k + 1) * size]
                row = jnp.minimum(rows_ref[0, 2 * two + k, face], block_rows - 1)
                field_ref[row] = field_ref[row] + fold(part, width)


def link_kernel(dev_count, pad, rows_ref, base_ref, links_ref, *refs):
    count = len(MATCHINGS)
    far_refs, split_ref, out_refs, field_ref = refs[:count], refs[count], refs[count + 1 : -1], refs[-1]
    add_links(dev_count, rows_ref, base_ref, links_ref, far_refs, field_ref)
    send_rows(dev_count, rows_ref, field_ref, out_refs)
    split_field(field_ref, split_ref, pad)


def gram_rows(left, split_refs, cols):
    width = split_refs[0].shape[0] // PIECES
    right = [ref[piece * width : (piece + 1) * width, cols] for piece in range(PIECES) for ref in split_refs]
    fill = [jnp.zeros_like(right[0])] * (2 * 128 // width - len(right))
    return lax.dot_general(
        left, jnp.concatenate(right + fill, axis=0), (((1,), (1,)), ((), ())), preferred_element_type=F32
    )


def fold_lanes(value):
    first = value[:, :128]
    return value[:, 128:] + (first + pltpu.roll(first, 64, 1))


def gram_kernel(pad, split0, split1, split2, out_ref, total):
    rows, lanes = split0.shape
    width = rows // PIECES
    refs = (split0, split1, split2, split2)
    inner = lanes - 2 * pad * 128
    chunk = inner // 8
    total[...] = jnp.zeros_like(total)

    def body(step, carry):
        cols = pl.ds(pl.multiple_of(pad * 128 + step * chunk, 128), chunk)
        left = jnp.concatenate([ref[:, cols] for ref in refs[:3]], axis=0)
        total[...] += gram_rows(left, refs, cols)
        return carry

    lax.fori_loop(0, 8, body, 0)
    z = [fold_lanes(fold(total[rows * k : rows * (k + 1)], width)) for k in range(3)]
    lane = lax.broadcasted_iota(jnp.int32, z[0].shape, 1)
    out_ref[...] = jnp.where(
        lane < 2 * width,
        z[0],
        jnp.where(lane < 4 * width, pltpu.roll(z[1], width, 1), pltpu.roll(z[2], 2 * width, 1)),
    )


def last_link_kernel(dev_count, pad, rows_ref, base_ref, links_ref, split2, moments_ref, *refs):
    count = len(MATCHINGS)
    far_refs, split_ref, out_ref, field_ref = refs[:count], refs[count], refs[count + 1], refs[-1]
    add_links(dev_count, rows_ref, base_ref, links_ref, far_refs, field_ref)
    split_field(field_ref, split_ref, pad)
    rows, lanes = split2.shape
    width = rows // PIECES
    cols = slice(pad * 128, lanes - pad * 128)
    z = fold_lanes(fold(gram_rows(split2[:, cols], (split2, split2, split2, split_ref), cols), width))
    lane = lax.broadcasted_iota(jnp.int32, z.shape, 1)
    mine = jnp.where(lane < 5 * width, moments_ref[...], pltpu.roll(z, 2 * width, 1))
    mine = jnp.where(lane < 6 * width, mine, 0.0)
    for peer in range(out_ref.shape[0]):
        out_ref[peer] = mine


def finish_kernel(pad, gathered_ref, split0, split1, split2, split3, solution_ref, residual_ref):
    peers, width, lanes = gathered_ref.shape
    block_rows = solution_ref.shape[0]
    moments = gathered_ref[0]
    for peer in range(1, peers):
        moments = moments + gathered_ref[peer]
    table = [pltpu.roll(moments, lanes - width * (k + 1), 1) for k in range(ITERS)] + [moments]
    table = jnp.concatenate(table, axis=0)
    lane = lax.broadcasted_iota(jnp.int32, (1, lanes), 1)
    for k in range(ITERS * width):
        row = table[k : k + 1, :]
        column = table[:, k : k + 1] * (1.0 / table[k : k + 1, k : k + 1])
        table = jnp.where(lane == k, column, table - column * row)
    coeffs = table[ITERS * width :]
    lane = lax.broadcasted_iota(jnp.int32, coeffs.shape, 1)
    unit = (lane == lax.broadcasted_iota(jnp.int32, coeffs.shape, 0)).astype(F32)
    for_solution = jnp.where(lane < ITERS * width, coeffs, 0.0)
    for_residual = jnp.where(lane < width, unit, jnp.where(lane < LEVELS * width, -pltpu.roll(coeffs, width, 1), 0.0))
    both = jnp.concatenate([for_solution, for_residual], axis=0)
    both = jnp.concatenate([both + pltpu.roll(both, 64, 1), both], axis=1)[:, : PIECES * LEVELS * width]
    left = jnp.concatenate(pieces_of(both), axis=0)
    refs = (split0, split1, split2, split3)
    step = 4

    def body(index, carry):
        cols = pl.ds(pl.multiple_of((pad + index * step) * 128, 128), step * 128)
        right = [ref[piece * width : (piece + 1) * width, cols] for piece in range(PIECES) for ref in refs]
        total = fold(jnp.dot(left, jnp.concatenate(right, axis=0), preferred_element_type=F32), 2 * width)
        for k in range(step):
            solution_ref[index * step + k] = total[:width, k * 128 : (k + 1) * 128]
            residual_ref[index * step + k] = total[width:, k * 128 : (k + 1) * 128]
        return carry

    lax.fori_loop(0, block_rows // step, body, 0, unroll=2)


def shards(right_side, band_blocks, link_blocks, link_rows):
    dev_count = lax.axis_size("dom")
    block_rows, width, size = right_side.shape
    band = band_blocks.shape[1]
    half = band // 2
    faces, slots = link_rows.shape[1:]
    pairs = block_rows // 2
    count = len(MATCHINGS)
    message = jax.ShapeDtypeStruct((slots, width, size), F32)
    split = jax.ShapeDtypeStruct((PIECES * width, (block_rows + 2 * half) * size), BF16)
    field = jax.ShapeDtypeStruct(right_side.shape, F32)

    def exchange(messages):
        got = []
        for index, (pair, phase) in enumerate(MATCHINGS):
            got.append(lax.ppermute(messages[index], "dom", matching_pairs(dev_count, pair, phase)))
        return got

    hbm = [pl.BlockSpec(memory_space=pltpu.HBM)]
    right_side, band_blocks, link_blocks = (
        pltpu.with_memory_space_constraint(value, pltpu.HBM) for value in (right_side, band_blocks, link_blocks)
    )
    slot_rows = jnp.swapaxes(link_rows, 1, 2)
    messages = pl.pallas_call(
        functools.partial(first_send_kernel, dev_count),
        out_shape=[message] * count,
        in_specs=[smem()] + hbm,
        out_specs=vmem(count),
        scratch_shapes=[pltpu.SemaphoreType.DMA((count, slots))],
        compiler_params=params(8),
        name="first_send",
    )(slot_rows, right_side)
    far = exchange(messages)
    weights, links, split0, base = pl.pallas_call(
        functools.partial(prepare_kernel, half),
        out_shape=[
            pltpu.VMEM((pairs + 2, 2 * (band + 1), size, 2 * size), BF16),
            pltpu.VMEM((faces, slots // 2, 2 * size, 2 * size), BF16),
            split,
            field,
        ],
        in_specs=hbm * 3,
        out_specs=vmem(4),
        scratch_shapes=[
            pltpu.VMEM(right_side.shape, F32),
            pltpu.VMEM(band_blocks.shape, F32),
            pltpu.VMEM(link_blocks.shape[1:], F32),
            pltpu.SemaphoreType.DMA((pairs + 2,)),
        ],
        compiler_params=params(18),
        cost_estimate=pl.CostEstimate(flops=10**9, bytes_accessed=12 * 10**6, transcendentals=0),
        name="prepare",
    )(right_side, band_blocks, link_blocks)

    splits = [split0]
    for level in range(ITERS):
        if level > 0:
            base = pl.pallas_call(
                band_kernel,
                out_shape=field,
                in_specs=vmem(2),
                out_specs=vmem(1)[0],
                compiler_params=params(8),
                cost_estimate=pl.CostEstimate(flops=10**9, bytes_accessed=12 * 10**6, transcendentals=0),
                name="band",
            )(weights, splits[-1])
        if level + 1 < ITERS:
            outs = pl.pallas_call(
                functools.partial(link_kernel, dev_count, half),
                out_shape=[split] + [message] * count,
                in_specs=[smem()] + vmem(2 + count),
                out_specs=vmem(1 + count),
                scratch_shapes=[pltpu.VMEM(right_side.shape, F32)],
                compiler_params=params(8),
                name="link",
            )(slot_rows, base, links, *far)
            splits.append(outs[0])
            far = exchange(outs[1:])
    moments = pl.pallas_call(
        functools.partial(gram_kernel, half),
        out_shape=jax.ShapeDtypeStruct((width, 128), F32),
        in_specs=vmem(ITERS),
        out_specs=vmem(1)[0],
        scratch_shapes=[pltpu.VMEM((ITERS * PIECES * width, 256), F32)],
        compiler_params=params(8),
        cost_estimate=pl.CostEstimate(flops=10**9, bytes_accessed=4 * 10**6, transcendentals=0),
        name="gram",
    )(*splits)
    split3, mine = pl.pallas_call(
        functools.partial(last_link_kernel, dev_count, half),
        out_shape=[split, jax.ShapeDtypeStruct((dev_count, width, 128), F32)],
        in_specs=[smem()] + vmem(4 + count),
        out_specs=vmem(2),
        scratch_shapes=[pltpu.VMEM(right_side.shape, F32)],
        compiler_params=params(8),
        name="last_link",
    )(slot_rows, base, links, splits[-1], moments, *far)
    splits.append(split3)
    gathered = lax.all_to_all(mine, "dom", 0, 0)
    return pl.pallas_call(
        functools.partial(finish_kernel, half),
        out_shape=[field, field],
        in_specs=vmem(1 + LEVELS),
        out_specs=vmem(2),
        compiler_params=params(8),
        name="finish",
    )(gathered, *splits)


def solution(mesh):
    in_specs = (
        P("dom", None, None),
        P("dom", None, None, None),
        P("dom", None, None, None, None),
        P("dom", None, None),
    )
    out_specs = (P("dom", None, None), P("dom", None, None))
    return jax.shard_map(
        lambda *args: tuple(shards(*args)), mesh=mesh, in_specs=in_specs, out_specs=out_specs, check_vma=False
    )
```

```python
import functools

import jax
import jax.numpy as jnp
from jax import lax
from jax.experimental import pallas as pl
from jax.experimental.pallas import tpu as pltpu
from jax.sharding import PartitionSpec as P


ITERS = 3
TRUSTED_PIVOT = 0.008
HIGHEST = lax.Precision.HIGHEST
LEVELS = ITERS + 1
PIECES = 3
F32 = jnp.float32
BF16 = jnp.bfloat16
MIB = 1 << 20

MATCHINGS = ((0, 1), (1, 1), (2, 1), (2, 0), (1, 0), (0, 0))


def offsets(dev_count):
    return (1, dev_count // 16, dev_count // 4)


def matching_pairs(dev_count, pair, phase):
    off = offsets(dev_count)[pair]
    return [
        (i, (i + off) % dev_count if (i // off + phase) % 2 == 0 else (i - off) % dev_count)
        for i in range(dev_count)
    ]


def matching_face(dev_count, pair, phase):
    me = lax.axis_index("dom")
    return 2 * pair + lax.rem(me // offsets(dev_count)[pair] + phase, 2)


def pieces_of(value):
    high = value.astype(BF16)
    rest = value - high.astype(F32)
    mid = rest.astype(BF16)
    low = (rest - mid.astype(F32)).astype(BF16)
    return high, mid, low


def vmem(count):
    return [pl.BlockSpec(memory_space=pltpu.VMEM)] * count


def smem():
    return pl.BlockSpec(memory_space=pltpu.SMEM)


def params(mib):
    return pltpu.CompilerParams(vmem_limit_bytes=mib * MIB)


def send_rows(dev_count, rows_ref, field_ref, out_refs):
    block_rows = field_ref.shape[0]
    for (pair, phase), out_ref in zip(MATCHINGS, out_refs):
        face = matching_face(dev_count, pair, phase)
        for slot in range(rows_ref.shape[1]):
            row = jnp.minimum(rows_ref[0, slot, face], block_rows - 1)
            out_ref[slot] = field_ref[row]


def split_field(field_ref, split_ref, pad):
    block_rows, width, size = field_ref.shape
    zero = jnp.zeros((split_ref.shape[0], pad * size), BF16)
    split_ref[:, : pad * size] = zero
    split_ref[:, (pad + block_rows) * size :] = zero
    for row in range(block_rows):
        cols = slice((pad + row) * size, (pad + row + 1) * size)
        for piece, value in enumerate(pieces_of(field_ref[row])):
            split_ref[piece * width : (piece + 1) * width, cols] = value


def first_send_kernel(dev_count, rows_hbm, field_hbm, *refs):
    out_refs, (rows_ref, field_ref, sems) = refs[:-3], refs[-3:]
    fetch_field = pltpu.make_async_copy(field_hbm, field_ref, sems.at[0])
    fetch_rows = pltpu.make_async_copy(rows_hbm, rows_ref, sems.at[1])
    fetch_field.start()
    fetch_rows.start()
    fetch_rows.wait()
    fetch_field.wait()
    send_rows(dev_count, rows_ref, field_ref, out_refs)


def fold(value, width):
    total = value[(PIECES - 1) * width : PIECES * width]
    for piece in range(PIECES - 2, -1, -1):
        total = total + value[piece * width : (piece + 1) * width]
    return total


def pair_product(weights_ref, split_ref, out_ref, pair):
    _, width, size = out_ref.shape
    depth = weights_ref.shape[1] * size
    start = pl.multiple_of(pair * 2 * size, 2 * size)
    rows = split_ref[:, pl.ds(start, depth // 2)]
    both = jnp.concatenate([rows, rows], axis=1)
    weights = weights_ref[pair + 1].reshape(depth, 2 * size)
    total = fold(jnp.dot(both, weights, preferred_element_type=F32), width)
    out_ref[2 * pair] = total[:, :size]
    out_ref[2 * pair + 1] = total[:, size:]


def band_kernel(weights_ref, split_ref, out_ref):
    def body(pair, carry):
        pair_product(weights_ref, split_ref, out_ref, pair)
        return carry

    lax.fori_loop(0, out_ref.shape[0] // 2, body, 0, unroll=4)


def prepare_kernel(
    half, field_hbm, band_hbm, link_hbm, weights_ref, links_ref, split_ref, out_ref, field_ref, band_ref, link_ref, sems
):
    block_rows, band, size, _ = band_ref.shape
    faces, count = link_ref.shape[:2]
    pairs = block_rows // 2
    span = band + 1
    copies = [pltpu.make_async_copy(field_hbm, field_ref, sems.at[pairs])]
    copies += [
        pltpu.make_async_copy(band_hbm.at[pl.ds(2 * pair, 2)], band_ref.at[pl.ds(2 * pair, 2)], sems.at[pair])
        for pair in range(pairs)
    ]
    copies.append(pltpu.make_async_copy(link_hbm.at[0], link_ref, sems.at[pairs + 1]))
    for copy in copies:
        copy.start()
    wide = jnp.zeros((size, 2 * size), BF16)
    for copy in range(2):
        for place in range(half):
            weights_ref[1, copy * span + place] = wide
            weights_ref[pairs, copy * span + span - 1 - place] = wide
        for pair in range(1, pairs + 1):
            weights_ref[pair, copy * span, :, size:] = wide[:, :size]
            weights_ref[pair, copy * span + span - 1, :, :size] = wide[:, :size]
    copies[0].wait()
    split_field(field_ref, split_ref, half)

    def convert(step, carry):
        here = pl.ds(2 * step, 2)
        pltpu.make_async_copy(band_hbm.at[here], band_ref.at[here], sems.at[step]).wait()
        for even in range(2):
            for k in range(band):
                shift = (even + k - half) // 2
                col = (even + k - half) % 2
                place = even + half - 2 * shift
                block = band_ref[2 * step + even, k]
                high = block.astype(BF16)
                low = (block - high.astype(F32)).astype(BF16)
                cols = slice(col * size, (col + 1) * size)
                weights_ref[step + shift + 1, place, :, cols] = high
                weights_ref[step + shift + 1, span + place, :, cols] = low
        pair_product(weights_ref, split_ref, out_ref, jnp.maximum(step - 1, 0))
        return carry

    lax.fori_loop(0, pairs, convert, 0)
    pair_product(weights_ref, split_ref, out_ref, pairs - 1)
    copies[-1].wait()

    def convert_links(face, carry):
        for slot in range(count):
            block = link_ref[face, slot].T
            high = block.astype(BF16)
            low = (block - high.astype(F32)).astype(BF16)
            cols = slice(slot % 2 * size, (slot % 2 + 1) * size)
            links_ref[face, slot // 2, :size, cols] = high
            links_ref[face, slot // 2, size:, cols] = low
        return carry

    lax.fori_loop(0, faces, convert_links, 0)


def add_links(dev_count, rows_ref, base_ref, links_ref, far_refs, field_ref):
    block_rows, width, size = base_ref.shape
    field_ref[...] = base_ref[...]
    for (pair, phase), far_ref in zip(MATCHINGS, far_refs):
        face = matching_face(dev_count, pair, phase)
        for two in range(far_ref.shape[0] // 2):
            stacked = []
            for slot in (2 * two, 2 * two + 1):
                stacked.extend(pieces_of(far_ref[slot]))
            rows = jnp.concatenate(stacked, axis=0)
            both = jnp.concatenate([rows, rows], axis=1)
            product = jnp.dot(both, links_ref[face, two], preferred_element_type=F32)
            for k in range(2):
                part = product[k * PIECES * width : (k + 1) * PIECES * width, k * size : (k + 1) * size]
                row = jnp.minimum(rows_ref[0, 2 * two + k, face], block_rows - 1)
                field_ref[row] = field_ref[row] + fold(part, width)


def link_kernel(dev_count, pad, rows_ref, base_ref, links_ref, *refs):
    count = len(MATCHINGS)
    far_refs, split_ref, out_refs, field_ref = refs[:count], refs[count], refs[count + 1 : -1], refs[-1]
    add_links(dev_count, rows_ref, base_ref, links_ref, far_refs, field_ref)
    send_rows(dev_count, rows_ref, field_ref, out_refs)
    split_field(field_ref, split_ref, pad)


def gram_rows(left, split_refs, cols):
    width = split_refs[0].shape[0] // PIECES
    right = [ref[piece * width : (piece + 1) * width, cols] for piece in range(PIECES) for ref in split_refs]
    fill = [jnp.zeros_like(right[0])] * (2 * 128 // width - len(right))
    return lax.dot_general(
        left, jnp.concatenate(right + fill, axis=0), (((1,), (1,)), ((), ())), preferred_element_type=F32
    )


def fold_lanes(value):
    first = value[:, :128]
    return value[:, 128:] + (first + pltpu.roll(first, 64, 1))


def gram_kernel(pad, split0, split1, split2, out_ref, total):
    rows, lanes = split0.shape
    width = rows // PIECES
    refs = (split0, split1, split2, split2)
    inner = lanes - 2 * pad * 128
    chunk = inner // 8
    total[...] = jnp.zeros_like(total)

    def body(step, carry):
        cols = pl.ds(pl.multiple_of(pad * 128 + step * chunk, 128), chunk)
        left = jnp.concatenate([ref[:, cols] for ref in refs[:3]], axis=0)
        total[...] += gram_rows(left, refs, cols)
        return carry

    lax.fori_loop(0, 8, body, 0)
    z = [fold_lanes(fold(total[rows * k : rows * (k + 1)], width)) for k in range(3)]
    lane = lax.broadcasted_iota(jnp.int32, z[0].shape, 1)
    out_ref[...] = jnp.where(
        lane < 2 * width,
        z[0],
        jnp.where(lane < 4 * width, pltpu.roll(z[1], width, 1), pltpu.roll(z[2], 2 * width, 1)),
    )


def places(width, lanes):
    row = lax.broadcasted_iota(jnp.int32, (width, lanes), 0)
    lane = lax.broadcasted_iota(jnp.int32, (width, lanes), 1)
    return row, lane, lane % width


def pack(moments):
    width, lanes = moments.shape
    row, lane, col = places(width, lanes)
    odd = pltpu.roll(moments, lanes - width, 1)
    tiles = jnp.where(row <= col, moments, odd)
    diagonal = jnp.sum(jnp.where(row == col, odd, 0.0), axis=0, keepdims=True)
    half = width // 2
    row, lane = row[:half], lane[:half]
    packed = jnp.where(lane % (2 * width) < width, tiles[:half], pltpu.roll(tiles[half:], width, 1))
    packed = jnp.where(lane < 6 * width, packed, 0.0)
    for k in range(3):
        here = (row == k) & (lane >= 6 * width) & (lane < 7 * width)
        packed = jnp.where(here, pltpu.roll(diagonal, (6 - 2 * k) * width, 1), packed)
    return packed


def unpack(packed):
    half, lanes = packed.shape
    width = 2 * half
    row, lane, col = places(width, lanes)
    tiles = jnp.concatenate([packed, pltpu.roll(packed, lanes - width, 1)], axis=0)
    turned = jnp.concatenate([tiles, jnp.zeros((lanes - width, lanes), F32)], axis=0).T
    mirror = jnp.zeros_like(tiles)
    diagonal = jnp.zeros_like(tiles)
    for k in range(3):
        here = (lane >= 2 * k * width) & (lane < (2 * k + 1) * width)
        part = turned[2 * k * width : (2 * k + 1) * width]
        mirror = jnp.where(here, pltpu.roll(part, 2 * k * width, 1) if k else part, mirror)
        diagonal = jnp.where(here, pltpu.roll(packed[k : k + 1], lanes - (6 - 2 * k) * width, 1), diagonal)
    even = jnp.where(row <= col, tiles, mirror)
    odd = jnp.where(row > col, tiles, jnp.where(row < col, mirror, diagonal))
    both = jnp.where(lane % (2 * width) < width, even, pltpu.roll(odd, width, 1))
    return jnp.where(lane < 6 * width, both, 0.0)


def last_link_kernel(dev_count, pad, rows_ref, base_ref, links_ref, split2, moments_ref, *refs):
    count = len(MATCHINGS)
    far_refs, split_ref, out_ref, field_ref = refs[:count], refs[count], refs[count + 1], refs[-1]
    add_links(dev_count, rows_ref, base_ref, links_ref, far_refs, field_ref)
    split_field(field_ref, split_ref, pad)
    rows, lanes = split2.shape
    width = rows // PIECES
    cols = slice(pad * 128, lanes - pad * 128)
    z = fold_lanes(fold(gram_rows(split2[:, cols], (split2, split2, split2, split_ref), cols), width))
    lane = lax.broadcasted_iota(jnp.int32, z.shape, 1)
    mine = jnp.where(lane < 5 * width, moments_ref[...], pltpu.roll(z, 2 * width, 1))
    mine = pack(mine)
    for peer in range(out_ref.shape[0]):
        out_ref[peer] = mine


def finish_kernel(pad, gathered_ref, split0, split1, split2, split3, solution_ref, residual_ref, doubt_ref):
    peers, half, lanes = gathered_ref.shape
    width = 2 * half
    block_rows = solution_ref.shape[0]
    sums = [gathered_ref[peer] for peer in range(peers)]
    while len(sums) > 1:
        sums = [sum(sums[k + 1 : k + 2], sums[k]) for k in range(0, len(sums), 2)]
    moments = unpack(sums[0])
    table = [pltpu.roll(moments, lanes - width * (k + 1), 1) for k in range(ITERS)] + [moments]
    table = jnp.concatenate(table, axis=0)
    lane = lax.broadcasted_iota(jnp.int32, (1, lanes), 1)
    across = lax.broadcasted_iota(jnp.int32, table.shape, 1) == lax.broadcasted_iota(jnp.int32, table.shape, 0)
    diagonal = jnp.sum(jnp.where(across, table, 0.0), axis=0, keepdims=True)
    pivots = jnp.zeros((1, lanes), F32)
    for k in range(0, ITERS * width, 2):
        if k and k % 8 == 0:
            table = table[8:]
        at = k % 8
        first, second = table[at : at + 1], table[at + 1 : at + 2]
        left, right = table[:, k : k + 1], table[:, k + 1 : k + 2]
        p11, p12 = left[at : at + 1], right[at : at + 1]
        p21, p22 = left[at + 1 : at + 2], right[at + 1 : at + 2]
        det = p11 * p22 - p12 * p21
        inverse = 1.0 / det
        pivots = jnp.where(lane == k, p11, jnp.where(lane == k + 1, det / p11, pivots))
        left, right = (left * p22 - right * p21) * inverse, (right * p11 - left * p12) * inverse
        rest = table - left * first - right * second
        table = jnp.where(lane == k, left, jnp.where(lane == k + 1, right, rest))
    trusted = (pivots > TRUSTED_PIVOT * diagonal) & (pivots < jnp.inf)
    used = lane < ITERS * width
    doubt = jnp.where(used & jnp.logical_not(trusted), 1.0, 0.0)
    doubt_ref[...] = jnp.broadcast_to(jnp.max(doubt, axis=1, keepdims=True), doubt_ref.shape)
    coeffs = table[-width:]
    lane = lax.broadcasted_iota(jnp.int32, coeffs.shape, 1)
    unit = (lane == lax.broadcasted_iota(jnp.int32, coeffs.shape, 0)).astype(F32)
    for_solution = jnp.where(lane < ITERS * width, coeffs, 0.0)
    for_residual = jnp.where(lane < width, unit, jnp.where(lane < LEVELS * width, -pltpu.roll(coeffs, width, 1), 0.0))
    both = jnp.concatenate([for_solution, for_residual], axis=0)
    both = jnp.concatenate([both + pltpu.roll(both, 64, 1), both], axis=1)[:, : PIECES * LEVELS * width]
    left = jnp.concatenate(pieces_of(both), axis=0)
    refs = (split0, split1, split2, split3)
    step = 4

    def body(index, carry):
        cols = pl.ds(pl.multiple_of((pad + index * step) * 128, 128), step * 128)
        right = [ref[piece * width : (piece + 1) * width, cols] for piece in range(PIECES) for ref in refs]
        total = fold(jnp.dot(left, jnp.concatenate(right, axis=0), preferred_element_type=F32), 2 * width)
        for k in range(step):
            solution_ref[index * step + k] = total[:width, k * 128 : (k + 1) * 128]
            residual_ref[index * step + k] = total[width:, k * 128 : (k + 1) * 128]
        return carry

    lax.fori_loop(0, block_rows // step, body, 0, unroll=2)


def gram_matrix(left, right):
    return lax.psum(jnp.einsum("nsi,nti->st", left, right, precision=HIGHEST), "dom")


def mix_columns(field, coeffs):
    return jnp.einsum("nsi,st->nti", field, coeffs, precision=HIGHEST)


def solve_gram(matrix, target):
    factor = jnp.linalg.cholesky(0.5 * (matrix + matrix.T))
    return jax.scipy.linalg.cho_solve((factor, True), target)


def plain_kernel(field_ref, band_ref, out_ref):
    row = pl.program_id(0)
    total = jnp.zeros(out_ref.shape[1:], F32)
    for k in range(band_ref.shape[1]):
        total += lax.dot_general(
            field_ref[row + k], band_ref[0, k], (((1,), (1,)), ((), ())), precision=HIGHEST, preferred_element_type=F32
        )
    out_ref[0] = total


def apply_operator(field, band_blocks, link_blocks, link_rows):
    dev_count = lax.axis_size("dom")
    block_rows, band = band_blocks.shape[:2]
    half = band // 2
    picks = (link_rows[0][:, :, None] == jnp.arange(block_rows, dtype=jnp.int32)).astype(field.dtype)
    padded = jnp.pad(field, ((half, half), (0, 0), (0, 0)))
    total = pl.pallas_call(
        plain_kernel,
        out_shape=jax.ShapeDtypeStruct(field.shape, F32),
        grid=(block_rows,),
        in_specs=[
            pl.BlockSpec(padded.shape, lambda r: (0, 0, 0)),
            pl.BlockSpec((1, *band_blocks.shape[1:]), lambda r: (r, 0, 0, 0)),
        ],
        out_specs=pl.BlockSpec((1, *field.shape[1:]), lambda r: (r, 0, 0)),
        compiler_params=params(8),
        name="plain",
    )(padded, band_blocks)
    for face in range(link_rows.shape[1]):
        by = offsets(dev_count)[face // 2] * (1 - 2 * (face % 2))
        source = jnp.einsum("hr,rsi->hsi", picks[face ^ 1], field, precision=HIGHEST)
        far = lax.ppermute(source, "dom", [(i, (i - by) % dev_count) for i in range(dev_count)])
        part = jnp.einsum("hsj,hij->hsi", far, link_blocks[0, face], precision=HIGHEST)
        total += jnp.einsum("hr,hsi->rsi", picks[face], part, precision=HIGHEST)
    return total


def classical(right_side, band_blocks, link_blocks, link_rows):
    def iterate(_, state):
        value, rest, direction, squares = state
        image = apply_operator(direction, band_blocks, link_blocks, link_rows)
        alpha = solve_gram(gram_matrix(direction, image), squares)
        value = value + mix_columns(direction, alpha)
        rest = rest - mix_columns(image, alpha)
        fresh = gram_matrix(rest, rest)
        direction = rest + mix_columns(direction, solve_gram(squares, fresh))
        return value, rest, direction, fresh

    start = (jnp.zeros_like(right_side), right_side, right_side, gram_matrix(right_side, right_side))
    return lax.fori_loop(0, ITERS, iterate, start)[:2]


def shards(*args):
    right_side, band_blocks, link_blocks, link_rows = args
    dev_count = lax.axis_size("dom")
    block_rows, width, size = right_side.shape
    band = band_blocks.shape[1]
    half = band // 2
    faces, slots = link_rows.shape[1:]
    pairs = block_rows // 2
    count = len(MATCHINGS)
    message = jax.ShapeDtypeStruct((slots, width, size), F32)
    split = jax.ShapeDtypeStruct((PIECES * width, (block_rows + 2 * half) * size), BF16)
    field = jax.ShapeDtypeStruct(right_side.shape, F32)

    def exchange(messages):
        got = []
        for index, (pair, phase) in enumerate(MATCHINGS):
            got.append(lax.ppermute(messages[index], "dom", matching_pairs(dev_count, pair, phase)))
        return got

    hbm = [pl.BlockSpec(memory_space=pltpu.HBM)]
    right_side, band_blocks, link_blocks = (
        pltpu.with_memory_space_constraint(value, pltpu.HBM) for value in (right_side, band_blocks, link_blocks)
    )
    slot_rows = pltpu.with_memory_space_constraint(jnp.swapaxes(link_rows, 1, 2), pltpu.HBM)
    messages = pl.pallas_call(
        functools.partial(first_send_kernel, dev_count),
        out_shape=[message] * count,
        in_specs=hbm * 2,
        out_specs=vmem(count),
        scratch_shapes=[
            pltpu.SMEM(slot_rows.shape, jnp.int32),
            pltpu.VMEM(right_side.shape, F32),
            pltpu.SemaphoreType.DMA((2,)),
        ],
        compiler_params=params(8),
        name="first_send",
    )(slot_rows, right_side)
    far = exchange(messages)
    weights, links, split0, base = pl.pallas_call(
        functools.partial(prepare_kernel, half),
        out_shape=[
            pltpu.VMEM((pairs + 2, 2 * (band + 1), size, 2 * size), BF16),
            pltpu.VMEM((faces, slots // 2, 2 * size, 2 * size), BF16),
            split,
            field,
        ],
        in_specs=hbm * 3,
        out_specs=vmem(4),
        scratch_shapes=[
            pltpu.VMEM(right_side.shape, F32),
            pltpu.VMEM(band_blocks.shape, F32),
            pltpu.VMEM(link_blocks.shape[1:], F32),
            pltpu.SemaphoreType.DMA((pairs + 2,)),
        ],
        compiler_params=params(18),
        cost_estimate=pl.CostEstimate(flops=10**9, bytes_accessed=12 * 10**6, transcendentals=0),
        name="prepare",
    )(right_side, band_blocks, link_blocks)

    splits = [split0]
    for level in range(ITERS):
        if level > 0:
            base = pl.pallas_call(
                band_kernel,
                out_shape=field,
                in_specs=vmem(2),
                out_specs=vmem(1)[0],
                compiler_params=params(8),
                cost_estimate=pl.CostEstimate(flops=10**9, bytes_accessed=12 * 10**6, transcendentals=0),
                name="band",
            )(weights, splits[-1])
        if level + 1 < ITERS:
            outs = pl.pallas_call(
                functools.partial(link_kernel, dev_count, half),
                out_shape=[split] + [message] * count,
                in_specs=[smem()] + vmem(2 + count),
                out_specs=vmem(1 + count),
                scratch_shapes=[pltpu.VMEM(right_side.shape, F32)],
                compiler_params=params(8),
                name="link",
            )(slot_rows, base, links, *far)
            splits.append(outs[0])
            far = exchange(outs[1:])
    moments = pl.pallas_call(
        functools.partial(gram_kernel, half),
        out_shape=jax.ShapeDtypeStruct((width, 128), F32),
        in_specs=vmem(ITERS),
        out_specs=vmem(1)[0],
        scratch_shapes=[pltpu.VMEM((ITERS * PIECES * width, 256), F32)],
        compiler_params=params(8),
        cost_estimate=pl.CostEstimate(flops=10**9, bytes_accessed=4 * 10**6, transcendentals=0),
        name="gram",
    )(*splits)
    split3, mine = pl.pallas_call(
        functools.partial(last_link_kernel, dev_count, half),
        out_shape=[split, jax.ShapeDtypeStruct((dev_count, width // 2, 128), F32)],
        in_specs=[smem()] + vmem(4 + count),
        out_specs=vmem(2),
        scratch_shapes=[pltpu.VMEM(right_side.shape, F32)],
        compiler_params=params(8),
        name="last_link",
    )(slot_rows, base, links, splits[-1], moments, *far)
    splits.append(split3)
    gathered = lax.all_to_all(mine, "dom", 0, 0)
    value, rest, doubt = pl.pallas_call(
        functools.partial(finish_kernel, half),
        out_shape=[field, field, jax.ShapeDtypeStruct((8, 128), F32)],
        in_specs=vmem(1 + LEVELS),
        out_specs=vmem(3),
        compiler_params=params(8),
        name="finish",
    )(gathered, *splits)
    again = lambda state: state[0][0, 0] > 0.0

    def redo(state):
        held, flag = lax.optimization_barrier((args, state[0]))
        return 0.0 * flag, *classical(*held)

    return lax.while_loop(again, redo, (doubt, value, rest))[1:]


def solution(mesh):
    in_specs = (
        P("dom", None, None),
        P("dom", None, None, None),
        P("dom", None, None, None, None),
        P("dom", None, None),
    )
    out_specs = (P("dom", None, None), P("dom", None, None))
    return jax.shard_map(
        lambda *args: tuple(shards(*args)), mesh=mesh, in_specs=in_specs, out_specs=out_specs, check_vma=False
    )
```

```python
import functools

import jax
import jax.numpy as jnp
from jax import lax
from jax.experimental import pallas as pl
from jax.experimental.pallas import tpu as pltpu
from jax.sharding import PartitionSpec as P


ITERS = 3
TRUSTED_PIVOT = 0.008
AHEAD = 3
HIGHEST = lax.Precision.HIGHEST
LEVELS = ITERS + 1
PIECES = 3
F32 = jnp.float32
BF16 = jnp.bfloat16
MIB = 1 << 20

MATCHINGS = ((0, 1), (1, 1), (2, 1), (2, 0), (1, 0), (0, 0))


def offsets(dev_count):
    return (1, dev_count // 16, dev_count // 4)


def matching_pairs(dev_count, pair, phase):
    off = offsets(dev_count)[pair]
    return [
        (i, (i + off) % dev_count if (i // off + phase) % 2 == 0 else (i - off) % dev_count)
        for i in range(dev_count)
    ]


def matching_face(dev_count, pair, phase):
    me = lax.axis_index("dom")
    return 2 * pair + lax.rem(me // offsets(dev_count)[pair] + phase, 2)


def pieces_of(value):
    high = value.astype(BF16)
    rest = value - high.astype(F32)
    mid = rest.astype(BF16)
    low = (rest - mid.astype(F32)).astype(BF16)
    return high, mid, low


def vmem(count):
    return [pl.BlockSpec(memory_space=pltpu.VMEM)] * count


def smem():
    return pl.BlockSpec(memory_space=pltpu.SMEM)


def params(mib):
    return pltpu.CompilerParams(vmem_limit_bytes=mib * MIB)


def send_rows(dev_count, rows_ref, field_ref, out_refs):
    block_rows = field_ref.shape[0]
    for (pair, phase), out_ref in zip(MATCHINGS, out_refs):
        face = matching_face(dev_count, pair, phase)
        for slot in range(rows_ref.shape[1]):
            row = jnp.minimum(rows_ref[0, slot, face], block_rows - 1)
            out_ref[slot] = field_ref[row]


def split_field(field_ref, split_ref, pad):
    block_rows, width, size = field_ref.shape
    zero = jnp.zeros((split_ref.shape[0], pad * size), BF16)
    split_ref[:, : pad * size] = zero
    split_ref[:, (pad + block_rows) * size :] = zero
    for row in range(block_rows):
        cols = slice((pad + row) * size, (pad + row + 1) * size)
        for piece, value in enumerate(pieces_of(field_ref[row])):
            split_ref[piece * width : (piece + 1) * width, cols] = value


def first_send_kernel(dev_count, rows_hbm, field_hbm, *refs):
    out_refs, (rows_ref, field_ref, sems) = refs[:-3], refs[-3:]
    fetch_field = pltpu.make_async_copy(field_hbm, field_ref, sems.at[0])
    fetch_rows = pltpu.make_async_copy(rows_hbm, rows_ref, sems.at[1])
    fetch_field.start()
    fetch_rows.start()
    fetch_rows.wait()
    fetch_field.wait()
    send_rows(dev_count, rows_ref, field_ref, out_refs)


def fold(value, width):
    total = value[(PIECES - 1) * width : PIECES * width]
    for piece in range(PIECES - 2, -1, -1):
        total = total + value[piece * width : (piece + 1) * width]
    return total


def pair_product(weights_ref, split_ref, out_ref, pair):
    _, width, size = out_ref.shape
    depth = weights_ref.shape[1] * size
    start = pl.multiple_of(pair * 2 * size, 2 * size)
    rows = split_ref[:, pl.ds(start, depth // 2)]
    both = jnp.concatenate([rows, rows], axis=1)
    weights = weights_ref[pair + 1].reshape(depth, 2 * size)
    total = fold(jnp.dot(both, weights, preferred_element_type=F32), width)
    out_ref[2 * pair] = total[:, :size]
    out_ref[2 * pair + 1] = total[:, size:]


def band_kernel(pad, weights_ref, field_ref, out_ref, split_ref):
    split_field(field_ref, split_ref, pad)

    def body(pair, carry):
        pair_product(weights_ref, split_ref, out_ref, pair)
        return carry

    lax.fori_loop(0, out_ref.shape[0] // 2, body, 0, unroll=4)


def prepare_kernel(
    half, field_hbm, band_hbm, link_hbm, weights_ref, links_ref, split_ref, out_ref, field_ref, band_ref, link_ref, sems
):
    block_rows, band, size, _ = band_ref.shape
    faces, count = link_ref.shape[:2]
    pairs = block_rows // 2
    span = band + 1
    copies = [pltpu.make_async_copy(field_hbm, field_ref, sems.at[pairs])]
    copies += [
        pltpu.make_async_copy(band_hbm.at[pl.ds(2 * pair, 2)], band_ref.at[pl.ds(2 * pair, 2)], sems.at[pair])
        for pair in range(pairs)
    ]
    copies.append(pltpu.make_async_copy(link_hbm.at[0], link_ref, sems.at[pairs + 1]))
    for copy in copies:
        copy.start()
    wide = jnp.zeros((size, 2 * size), BF16)
    for copy in range(2):
        for place in range(half):
            weights_ref[1, copy * span + place] = wide
            weights_ref[pairs, copy * span + span - 1 - place] = wide
        for pair in range(1, pairs + 1):
            weights_ref[pair, copy * span, :, size:] = wide[:, :size]
            weights_ref[pair, copy * span + span - 1, :, :size] = wide[:, :size]
    copies[0].wait()
    split_field(field_ref, split_ref, half)

    def convert(step, carry):
        here = pl.ds(2 * step, 2)
        pltpu.make_async_copy(band_hbm.at[here], band_ref.at[here], sems.at[step]).wait()
        pair_product(weights_ref, split_ref, out_ref, jnp.maximum(step - 2, 0))
        for even in range(2):
            for k in range(band):
                shift = (even + k - half) // 2
                col = (even + k - half) % 2
                place = even + half - 2 * shift
                block = band_ref[2 * step + even, k]
                high = block.astype(BF16)
                low = (block - high.astype(F32)).astype(BF16)
                cols = slice(col * size, (col + 1) * size)
                weights_ref[step + shift + 1, place, :, cols] = high
                weights_ref[step + shift + 1, span + place, :, cols] = low
        return carry

    lax.fori_loop(0, pairs, convert, 0)
    pair_product(weights_ref, split_ref, out_ref, pairs - 2)
    pair_product(weights_ref, split_ref, out_ref, pairs - 1)
    copies[-1].wait()

    def convert_links(face, carry):
        for slot in range(count):
            block = link_ref[face, slot].T
            high = block.astype(BF16)
            low = (block - high.astype(F32)).astype(BF16)
            cols = slice(slot % 2 * size, (slot % 2 + 1) * size)
            links_ref[face, slot // 2, :size, cols] = high
            links_ref[face, slot // 2, size:, cols] = low
        return carry

    lax.fori_loop(0, faces, convert_links, 0)


def add_links(dev_count, rows_ref, base_ref, links_ref, far_refs, field_ref):
    block_rows, width, size = base_ref.shape
    field_ref[...] = base_ref[...]
    for (pair, phase), far_ref in zip(MATCHINGS, far_refs):
        face = matching_face(dev_count, pair, phase)
        for two in range(far_ref.shape[0] // 2):
            stacked = []
            for slot in (2 * two, 2 * two + 1):
                stacked.extend(pieces_of(far_ref[slot]))
            rows = jnp.concatenate(stacked, axis=0)
            both = jnp.concatenate([rows, rows], axis=1)
            product = jnp.dot(both, links_ref[face, two], preferred_element_type=F32)
            for k in range(2):
                part = product[k * PIECES * width : (k + 1) * PIECES * width, k * size : (k + 1) * size]
                row = jnp.minimum(rows_ref[0, 2 * two + k, face], block_rows - 1)
                field_ref[row] = field_ref[row] + fold(part, width)


def link_kernel(dev_count, rows_ref, base_ref, links_ref, *refs):
    count = len(MATCHINGS)
    far_refs, field_ref, out_refs = refs[:count], refs[count], refs[count + 1 :]
    add_links(dev_count, rows_ref, base_ref, links_ref, far_refs, field_ref)
    send_rows(dev_count, rows_ref, field_ref, out_refs)


def gram(pad, left_refs, right_refs):
    rows, lanes = left_refs[0].shape
    width = rows // PIECES
    cols = slice(pad * 128, lanes - pad * 128)
    left = jnp.concatenate([ref[:, cols] for ref in left_refs], axis=0)
    right = [ref[piece * width : (piece + 1) * width, cols] for piece in range(PIECES) for ref in right_refs]
    right += [jnp.zeros_like(right[0])] * (128 // width - len(right))
    dims = (((1,), (1,)), ((), ()))
    product = lax.dot_general(left, jnp.concatenate(right, axis=0), dims, preferred_element_type=F32)
    step = len(right_refs) * width
    sums = []
    for k in range(len(left_refs)):
        part = fold(product[rows * k : rows * (k + 1)], width)
        total = part
        for piece in range(1, PIECES):
            total = total + pltpu.roll(part, 128 - piece * step, 1)
        sums.append(total)
    return sums


def lane_of(value):
    return lax.broadcasted_iota(jnp.int32, value.shape, 1)


def early_gram_kernel(pad, split0, split1, out_ref):
    width = out_ref.shape[0]
    first, second = gram(pad, (split0, split1), (split0, split1))
    out_ref[...] = jnp.where(lane_of(first) < 2 * width, first, pltpu.roll(second, width, 1))


def late_gram_kernel(pad, split1, split2, early_ref, out_ref):
    width = out_ref.shape[0]
    (late,) = gram(pad, (split2,), (split1, split2))
    out_ref[...] = jnp.where(lane_of(late) < 3 * width, early_ref[...], pltpu.roll(late, 3 * width, 1))


def places(width, lanes):
    row = lax.broadcasted_iota(jnp.int32, (width, lanes), 0)
    lane = lax.broadcasted_iota(jnp.int32, (width, lanes), 1)
    return row, lane, lane % width


def pack(moments):
    width, lanes = moments.shape
    row, lane, col = places(width, lanes)
    odd = pltpu.roll(moments, lanes - width, 1)
    tiles = jnp.where(row <= col, moments, odd)
    diagonal = jnp.sum(jnp.where(row == col, odd, 0.0), axis=0, keepdims=True)
    half = width // 2
    row, lane = row[:half], lane[:half]
    packed = jnp.where(lane % (2 * width) < width, tiles[:half], pltpu.roll(tiles[half:], width, 1))
    packed = jnp.where(lane < 6 * width, packed, 0.0)
    for k in range(3):
        here = (row == k) & (lane >= 6 * width) & (lane < 7 * width)
        packed = jnp.where(here, pltpu.roll(diagonal, (6 - 2 * k) * width, 1), packed)
    return packed


def unpack(packed):
    half, lanes = packed.shape
    width = 2 * half
    row, lane, col = places(width, lanes)
    tiles = jnp.concatenate([packed, pltpu.roll(packed, lanes - width, 1)], axis=0)
    turned = jnp.concatenate([tiles, jnp.zeros((lanes - width, lanes), F32)], axis=0).T
    mirror = jnp.zeros_like(tiles)
    diagonal = jnp.zeros_like(tiles)
    for k in range(3):
        here = (lane >= 2 * k * width) & (lane < (2 * k + 1) * width)
        part = turned[2 * k * width : (2 * k + 1) * width]
        mirror = jnp.where(here, pltpu.roll(part, 2 * k * width, 1) if k else part, mirror)
        diagonal = jnp.where(here, pltpu.roll(packed[k : k + 1], lanes - (6 - 2 * k) * width, 1), diagonal)
    even = jnp.where(row <= col, tiles, mirror)
    odd = jnp.where(row > col, tiles, jnp.where(row < col, mirror, diagonal))
    both = jnp.where(lane % (2 * width) < width, even, pltpu.roll(odd, width, 1))
    return jnp.where(lane < 6 * width, both, 0.0)


def last_link_kernel(dev_count, pad, rows_ref, base_ref, links_ref, split2, moments_ref, *refs):
    count = len(MATCHINGS)
    far_refs, split_ref, out_ref, field_ref = refs[:count], refs[count], refs[count + 1], refs[-1]
    add_links(dev_count, rows_ref, base_ref, links_ref, far_refs, field_ref)
    split_field(field_ref, split_ref, pad)
    width = moments_ref.shape[0]
    (last,) = gram(pad, (split2,), (split_ref,))
    mine = jnp.where(lane_of(last) < 5 * width, moments_ref[...], pltpu.roll(last, 5 * width, 1))
    mine = pack(mine)
    for peer in range(out_ref.shape[0]):
        out_ref[peer] = mine


def finish_kernel(pad, gathered_ref, split0, split1, split2, split3, solution_ref, residual_ref, doubt_ref):
    peers, half, lanes = gathered_ref.shape
    width = 2 * half
    block_rows = solution_ref.shape[0]
    sums = [gathered_ref[peer] for peer in range(peers)]
    while len(sums) > 1:
        sums = [sum(sums[k + 1 : k + 2], sums[k]) for k in range(0, len(sums), 2)]
    moments = unpack(sums[0])
    table = [pltpu.roll(moments, lanes - width * (k + 1), 1) for k in range(ITERS)] + [moments]
    table = jnp.concatenate(table, axis=0)
    lane = lax.broadcasted_iota(jnp.int32, (1, lanes), 1)
    across = lax.broadcasted_iota(jnp.int32, table.shape, 1) == lax.broadcasted_iota(jnp.int32, table.shape, 0)
    diagonal = jnp.sum(jnp.where(across, table, 0.0), axis=0, keepdims=True)
    pivots = jnp.zeros((1, lanes), F32)
    column = lambda k: jnp.broadcast_to(table[:, k : k + 1], table.shape)
    ahead = {k: (column(k), column(k + 1)) for k in range(0, 2 * AHEAD, 2)}
    for k in range(0, ITERS * width, 2):
        if k and k % 8 == 0:
            table = table[8:]
            ahead = {key: (one[8:], two[8:]) for key, (one, two) in ahead.items()}
        if k + 2 * AHEAD < ITERS * width:
            ahead[k + 2 * AHEAD] = (column(k + 2 * AHEAD), column(k + 2 * AHEAD + 1))
        at = k % 8
        left, right = ahead.pop(k)
        p11, p12 = left[at : at + 1], right[at : at + 1]
        p21, p22 = left[at + 1 : at + 2], right[at + 1 : at + 2]
        det = p11 * p22 - p12 * p21
        inverse = 1.0 / det
        pivots = jnp.where(lane == k, p11, jnp.where(lane == k + 1, det / p11, pivots))
        left, right = (left * p22 - right * p21) * inverse, (right * p11 - left * p12) * inverse
        clear = lambda value: value - left * value[at : at + 1] - right * value[at + 1 : at + 2]
        ahead = {key: (clear(one), clear(two)) for key, (one, two) in ahead.items()}
        table = jnp.where(lane == k, left, jnp.where(lane == k + 1, right, clear(table)))
    trusted = (pivots > TRUSTED_PIVOT * diagonal) & (pivots < jnp.inf)
    used = lane < ITERS * width
    doubt = jnp.where(used & jnp.logical_not(trusted), 1.0, 0.0)
    doubt_ref[0] = jnp.max(doubt).astype(jnp.int32)
    coeffs = table[-width:]
    lane = lax.broadcasted_iota(jnp.int32, coeffs.shape, 1)
    unit = (lane == lax.broadcasted_iota(jnp.int32, coeffs.shape, 0)).astype(F32)
    for_solution = jnp.where(lane < ITERS * width, coeffs, 0.0)
    for_residual = jnp.where(lane < width, unit, jnp.where(lane < LEVELS * width, -pltpu.roll(coeffs, width, 1), 0.0))
    both = jnp.concatenate([for_solution, for_residual], axis=0)
    both = jnp.concatenate([both + pltpu.roll(both, 64, 1), both], axis=1)[:, : PIECES * LEVELS * width]
    left = jnp.concatenate(pieces_of(both), axis=0)
    refs = (split0, split1, split2, split3)
    step = 4

    def body(index, carry):
        cols = pl.ds(pl.multiple_of((pad + index * step) * 128, 128), step * 128)
        right = [ref[piece * width : (piece + 1) * width, cols] for piece in range(PIECES) for ref in refs]
        total = fold(jnp.dot(left, jnp.concatenate(right, axis=0), preferred_element_type=F32), 2 * width)
        for k in range(step):
            solution_ref[index * step + k] = total[:width, k * 128 : (k + 1) * 128]
            residual_ref[index * step + k] = total[width:, k * 128 : (k + 1) * 128]
        return carry

    lax.fori_loop(0, block_rows // step, body, 0, unroll=2)


def gram_matrix(left, right):
    return lax.psum(jnp.einsum("nsi,nti->st", left, right, precision=HIGHEST), "dom")


def mix_columns(field, coeffs):
    return jnp.einsum("nsi,st->nti", field, coeffs, precision=HIGHEST)


def solve_gram(matrix, target):
    factor = jnp.linalg.cholesky(0.5 * (matrix + matrix.T))
    return jax.scipy.linalg.cho_solve((factor, True), target)


def plain_kernel(field_ref, band_ref, out_ref):
    row = pl.program_id(0)
    total = jnp.zeros(out_ref.shape[1:], F32)
    for k in range(band_ref.shape[1]):
        total += lax.dot_general(
            field_ref[row + k], band_ref[0, k], (((1,), (1,)), ((), ())), precision=HIGHEST, preferred_element_type=F32
        )
    out_ref[0] = total


def apply_operator(field, band_blocks, link_blocks, link_rows):
    dev_count = lax.axis_size("dom")
    block_rows, band = band_blocks.shape[:2]
    half = band // 2
    picks = (link_rows[0][:, :, None] == jnp.arange(block_rows, dtype=jnp.int32)).astype(field.dtype)
    padded = jnp.pad(field, ((half, half), (0, 0), (0, 0)))
    total = pl.pallas_call(
        plain_kernel,
        out_shape=jax.ShapeDtypeStruct(field.shape, F32),
        grid=(block_rows,),
        in_specs=[
            pl.BlockSpec(padded.shape, lambda r: (0, 0, 0)),
            pl.BlockSpec((1, *band_blocks.shape[1:]), lambda r: (r, 0, 0, 0)),
        ],
        out_specs=pl.BlockSpec((1, *field.shape[1:]), lambda r: (r, 0, 0)),
        compiler_params=params(8),
        name="plain",
    )(padded, band_blocks)
    for face in range(link_rows.shape[1]):
        by = offsets(dev_count)[face // 2] * (1 - 2 * (face % 2))
        source = jnp.einsum("hr,rsi->hsi", picks[face ^ 1], field, precision=HIGHEST)
        far = lax.ppermute(source, "dom", [(i, (i - by) % dev_count) for i in range(dev_count)])
        part = jnp.einsum("hsj,hij->hsi", far, link_blocks[0, face], precision=HIGHEST)
        total += jnp.einsum("hr,hsi->rsi", picks[face], part, precision=HIGHEST)
    return total


def classical(right_side, band_blocks, link_blocks, link_rows):
    def iterate(_, state):
        value, rest, direction, squares = state
        image = apply_operator(direction, band_blocks, link_blocks, link_rows)
        alpha = solve_gram(gram_matrix(direction, image), squares)
        value = value + mix_columns(direction, alpha)
        rest = rest - mix_columns(image, alpha)
        fresh = gram_matrix(rest, rest)
        direction = rest + mix_columns(direction, solve_gram(squares, fresh))
        return value, rest, direction, fresh

    start = (jnp.zeros_like(right_side), right_side, right_side, gram_matrix(right_side, right_side))
    return lax.fori_loop(0, ITERS, iterate, start)[:2]


def shards(*args):
    right_side, band_blocks, link_blocks, link_rows = args
    dev_count = lax.axis_size("dom")
    block_rows, width, size = right_side.shape
    band = band_blocks.shape[1]
    half = band // 2
    faces, slots = link_rows.shape[1:]
    pairs = block_rows // 2
    count = len(MATCHINGS)
    message = jax.ShapeDtypeStruct((slots, width, size), F32)
    split = jax.ShapeDtypeStruct((PIECES * width, (block_rows + 2 * half) * size), BF16)
    field = jax.ShapeDtypeStruct(right_side.shape, F32)

    def exchange(messages):
        got = []
        for index, (pair, phase) in enumerate(MATCHINGS):
            got.append(lax.ppermute(messages[index], "dom", matching_pairs(dev_count, pair, phase)))
        return got

    hbm = [pl.BlockSpec(memory_space=pltpu.HBM)]
    right_side, band_blocks, link_blocks = (
        pltpu.with_memory_space_constraint(value, pltpu.HBM) for value in (right_side, band_blocks, link_blocks)
    )
    slot_rows = pltpu.with_memory_space_constraint(jnp.swapaxes(link_rows, 1, 2), pltpu.HBM)
    messages = pl.pallas_call(
        functools.partial(first_send_kernel, dev_count),
        out_shape=[message] * count,
        in_specs=hbm * 2,
        out_specs=vmem(count),
        scratch_shapes=[
            pltpu.SMEM(slot_rows.shape, jnp.int32),
            pltpu.VMEM(right_side.shape, F32),
            pltpu.SemaphoreType.DMA((2,)),
        ],
        compiler_params=params(8),
        name="first_send",
    )(slot_rows, right_side)
    far = exchange(messages)
    weights, links, split0, base = pl.pallas_call(
        functools.partial(prepare_kernel, half),
        out_shape=[
            pltpu.VMEM((pairs + 2, 2 * (band + 1), size, 2 * size), BF16),
            pltpu.VMEM((faces, slots // 2, 2 * size, 2 * size), BF16),
            split,
            field,
        ],
        in_specs=hbm * 3,
        out_specs=vmem(4),
        scratch_shapes=[
            pltpu.VMEM(right_side.shape, F32),
            pltpu.VMEM(band_blocks.shape, F32),
            pltpu.VMEM(link_blocks.shape[1:], F32),
            pltpu.SemaphoreType.DMA((pairs + 2,)),
        ],
        compiler_params=params(18),
        cost_estimate=pl.CostEstimate(flops=10**9, bytes_accessed=12 * 10**6, transcendentals=0),
        name="prepare",
    )(right_side, band_blocks, link_blocks)

    splits = [split0]
    moments = None
    for level in range(ITERS):
        if level > 0:
            base, latest = pl.pallas_call(
                functools.partial(band_kernel, half),
                out_shape=[field, split],
                in_specs=vmem(2),
                out_specs=vmem(2),
                compiler_params=params(8),
                cost_estimate=pl.CostEstimate(flops=10**9, bytes_accessed=12 * 10**6, transcendentals=0),
                name="band",
            )(weights, values)
            splits.append(latest)
            late = level == ITERS - 1
            moments = pl.pallas_call(
                functools.partial(late_gram_kernel if late else early_gram_kernel, half),
                out_shape=jax.ShapeDtypeStruct((width, 128), F32),
                in_specs=vmem(2 + late),
                out_specs=vmem(1)[0],
                compiler_params=params(8),
                cost_estimate=pl.CostEstimate(flops=10**9, bytes_accessed=4 * 10**6, transcendentals=0),
                name="gram",
            )(*splits[-2:], *([moments] if late else []))
        if level + 1 < ITERS:
            values, *messages = pl.pallas_call(
                functools.partial(link_kernel, dev_count),
                out_shape=[field] + [message] * count,
                in_specs=[smem()] + vmem(2 + count),
                out_specs=vmem(1 + count),
                compiler_params=params(8),
                name="link",
            )(slot_rows, base, links, *far)
            far = exchange(messages)
    split3, mine = pl.pallas_call(
        functools.partial(last_link_kernel, dev_count, half),
        out_shape=[split, jax.ShapeDtypeStruct((dev_count, width // 2, 128), F32)],
        in_specs=[smem()] + vmem(4 + count),
        out_specs=vmem(2),
        scratch_shapes=[pltpu.VMEM(right_side.shape, F32)],
        compiler_params=params(8),
        name="last_link",
    )(slot_rows, base, links, splits[-1], moments, *far)
    splits.append(split3)
    gathered = lax.all_to_all(mine, "dom", 0, 0)
    value, rest, doubt = pl.pallas_call(
        functools.partial(finish_kernel, half),
        out_shape=[field, field, jax.ShapeDtypeStruct((1,), jnp.int32)],
        in_specs=vmem(1 + LEVELS),
        out_specs=vmem(2) + [smem()],
        compiler_params=params(8),
        name="finish",
    )(gathered, *splits)
    again = lambda state: state[0][0] > 0

    def redo(state):
        held, flag = lax.optimization_barrier((args, state[0]))
        return 0 * flag, *classical(*held)

    return lax.while_loop(again, redo, (doubt, value, rest))[1:]


def solution(mesh):
    in_specs = (
        P("dom", None, None),
        P("dom", None, None, None),
        P("dom", None, None, None, None),
        P("dom", None, None),
    )
    out_specs = (P("dom", None, None), P("dom", None, None))
    return jax.shard_map(
        lambda *args: tuple(shards(*args)), mesh=mesh, in_specs=in_specs, out_specs=out_specs, check_vma=False
    )
```

```python
import functools

import jax
import jax.numpy as jnp
from jax import lax
from jax.experimental import pallas as pl
from jax.experimental.pallas import tpu as pltpu
from jax.sharding import PartitionSpec as P


ITERS = 3
TRUSTED_PIVOT = 0.008
AHEAD = 3
HIGHEST = lax.Precision.HIGHEST
LEVELS = ITERS + 1
PIECES = 3
F32 = jnp.float32
BF16 = jnp.bfloat16
MIB = 1 << 20

MATCHINGS = ((0, 1), (1, 1), (2, 1), (2, 0), (1, 0), (0, 0))


def offsets(dev_count):
    return (1, dev_count // 16, dev_count // 4)


def matching_pairs(dev_count, pair, phase):
    off = offsets(dev_count)[pair]
    return [
        (i, (i + off) % dev_count if (i // off + phase) % 2 == 0 else (i - off) % dev_count)
        for i in range(dev_count)
    ]


def matching_face(dev_count, pair, phase):
    me = lax.axis_index("dom")
    return 2 * pair + lax.rem(me // offsets(dev_count)[pair] + phase, 2)


def pieces_of(value):
    high = value.astype(BF16)
    rest = value - high.astype(F32)
    mid = rest.astype(BF16)
    low = (rest - mid.astype(F32)).astype(BF16)
    return high, mid, low


def vmem(count):
    return [pl.BlockSpec(memory_space=pltpu.VMEM)] * count


def smem():
    return pl.BlockSpec(memory_space=pltpu.SMEM)


def params(mib):
    return pltpu.CompilerParams(vmem_limit_bytes=mib * MIB)


def send_rows(dev_count, rows_ref, field_ref, out_refs):
    block_rows = field_ref.shape[0]
    for (pair, phase), out_ref in zip(MATCHINGS, out_refs):
        face = matching_face(dev_count, pair, phase)
        for slot in range(rows_ref.shape[1]):
            row = jnp.minimum(rows_ref[0, slot, face], block_rows - 1)
            out_ref[slot] = field_ref[row]


def split_field(field_ref, split_ref, pad):
    block_rows, width, size = field_ref.shape
    zero = jnp.zeros((split_ref.shape[0], pad * size), BF16)
    split_ref[:, : pad * size] = zero
    split_ref[:, (pad + block_rows) * size :] = zero
    for row in range(block_rows):
        cols = slice((pad + row) * size, (pad + row + 1) * size)
        for piece, value in enumerate(pieces_of(field_ref[row])):
            split_ref[piece * width : (piece + 1) * width, cols] = value


def first_send_kernel(dev_count, rows_hbm, field_hbm, *refs):
    out_refs, (rows_ref, field_ref, sems) = refs[:-3], refs[-3:]
    fetch_field = pltpu.make_async_copy(field_hbm, field_ref, sems.at[0])
    fetch_rows = pltpu.make_async_copy(rows_hbm, rows_ref, sems.at[1])
    fetch_field.start()
    fetch_rows.start()
    fetch_rows.wait()
    fetch_field.wait()
    send_rows(dev_count, rows_ref, field_ref, out_refs)


def fold(value, width):
    total = value[(PIECES - 1) * width : PIECES * width]
    for piece in range(PIECES - 2, -1, -1):
        total = total + value[piece * width : (piece + 1) * width]
    return total


def pair_product(weights_ref, split_ref, out_ref, pair):
    _, width, size = out_ref.shape
    depth = weights_ref.shape[1] * size
    start = pl.multiple_of(pair * 2 * size, 2 * size)
    rows = split_ref[:, pl.ds(start, depth // 2)]
    both = jnp.concatenate([rows, rows], axis=1)
    weights = weights_ref[pair + 1].reshape(depth, 2 * size)
    total = fold(jnp.dot(both, weights, preferred_element_type=F32), width)
    out_ref[2 * pair] = total[:, :size]
    out_ref[2 * pair + 1] = total[:, size:]


def band_kernel(pad, weights_ref, field_ref, out_ref, split_ref):
    split_field(field_ref, split_ref, pad)

    def body(pair, carry):
        pair_product(weights_ref, split_ref, out_ref, pair)
        return carry

    lax.fori_loop(0, out_ref.shape[0] // 2, body, 0, unroll=4)


def prepare_kernel(
    half, field_hbm, band_hbm, link_hbm, weights_ref, links_ref, split_ref, out_ref, field_ref, band_ref, link_ref, total_ref, sems
):
    block_rows, band, size, _ = band_ref.shape
    faces, count = link_ref.shape[:2]
    pairs = block_rows // 2
    span = band + 1
    copies = [pltpu.make_async_copy(field_hbm, field_ref, sems.at[pairs])]
    copies += [
        pltpu.make_async_copy(band_hbm.at[pl.ds(2 * pair, 2)], band_ref.at[pl.ds(2 * pair, 2)], sems.at[pair])
        for pair in range(pairs)
    ]
    copies.append(pltpu.make_async_copy(link_hbm.at[0], link_ref, sems.at[pairs + 1]))
    for copy in copies:
        copy.start()
    wide = jnp.zeros((size, 2 * size), BF16)
    for copy in range(2):
        for place in range(half):
            weights_ref[1, copy * span + place] = wide
            weights_ref[pairs, copy * span + span - 1 - place] = wide
        for pair in range(1, pairs + 1):
            weights_ref[pair, copy * span, :, size:] = wide[:, :size]
            weights_ref[pair, copy * span + span - 1, :, :size] = wide[:, :size]
    total_ref[...] = jnp.zeros_like(total_ref)
    copies[0].wait()
    split_field(field_ref, split_ref, half)

    def convert(step, carry):
        here = pl.ds(2 * step, 2)
        pltpu.make_async_copy(band_hbm.at[here], band_ref.at[here], sems.at[step]).wait()
        for even in range(2):
            rows = split_ref[:, pl.ds(pl.multiple_of((half + 2 * step + even) * size, size), size)]
            both = jnp.concatenate([rows, rows], axis=1)
            for k in range(band):
                shift = (even + k - half) // 2
                col = (even + k - half) % 2
                place = even + half - 2 * shift
                block = band_ref[2 * step + even, k]
                high = block.astype(BF16)
                low = (block - high.astype(F32)).astype(BF16)
                cols = slice(col * size, (col + 1) * size)
                weights_ref[step + shift + 1, place, :, cols] = high
                weights_ref[step + shift + 1, span + place, :, cols] = low
                product = jnp.dot(both, jnp.concatenate([high, low], axis=0), preferred_element_type=F32)
                total_ref[2 * step + even + k] += fold(product, field_ref.shape[1])
        return carry

    lax.fori_loop(0, pairs, convert, 0)
    out_ref[...] = total_ref[pl.ds(half, block_rows)]
    copies[-1].wait()

    def convert_links(face, carry):
        for slot in range(count):
            block = link_ref[face, slot].T
            high = block.astype(BF16)
            low = (block - high.astype(F32)).astype(BF16)
            cols = slice(slot % 2 * size, (slot % 2 + 1) * size)
            links_ref[face, slot // 2, :size, cols] = high
            links_ref[face, slot // 2, size:, cols] = low
        return carry

    lax.fori_loop(0, faces, convert_links, 0)


def add_links(dev_count, rows_ref, base_ref, links_ref, far_refs, field_ref):
    block_rows, width, size = base_ref.shape
    field_ref[...] = base_ref[...]
    for (pair, phase), far_ref in zip(MATCHINGS, far_refs):
        face = matching_face(dev_count, pair, phase)
        for two in range(far_ref.shape[0] // 2):
            stacked = []
            for slot in (2 * two, 2 * two + 1):
                stacked.extend(pieces_of(far_ref[slot]))
            rows = jnp.concatenate(stacked, axis=0)
            both = jnp.concatenate([rows, rows], axis=1)
            product = jnp.dot(both, links_ref[face, two], preferred_element_type=F32)
            for k in range(2):
                part = product[k * PIECES * width : (k + 1) * PIECES * width, k * size : (k + 1) * size]
                row = jnp.minimum(rows_ref[0, 2 * two + k, face], block_rows - 1)
                field_ref[row] = field_ref[row] + fold(part, width)


def link_kernel(dev_count, rows_ref, base_ref, links_ref, *refs):
    count = len(MATCHINGS)
    far_refs, field_ref, out_refs = refs[:count], refs[count], refs[count + 1 :]
    add_links(dev_count, rows_ref, base_ref, links_ref, far_refs, field_ref)
    send_rows(dev_count, rows_ref, field_ref, out_refs)


def gram(pad, left_refs, right_refs):
    rows, lanes = left_refs[0].shape
    width = rows // PIECES
    cols = slice(pad * 128, lanes - pad * 128)
    left = jnp.concatenate([ref[:, cols] for ref in left_refs], axis=0)
    right = [ref[piece * width : (piece + 1) * width, cols] for piece in range(PIECES) for ref in right_refs]
    right += [jnp.zeros_like(right[0])] * (128 // width - len(right))
    dims = (((1,), (1,)), ((), ()))
    product = lax.dot_general(left, jnp.concatenate(right, axis=0), dims, preferred_element_type=F32)
    step = len(right_refs) * width
    sums = []
    for k in range(len(left_refs)):
        part = fold(product[rows * k : rows * (k + 1)], width)
        total = part
        for piece in range(1, PIECES):
            total = total + pltpu.roll(part, 128 - piece * step, 1)
        sums.append(total)
    return sums


def lane_of(value):
    return lax.broadcasted_iota(jnp.int32, value.shape, 1)


def early_gram_kernel(pad, split0, split1, out_ref):
    width = out_ref.shape[0]
    first, second = gram(pad, (split0, split1), (split0, split1))
    out_ref[...] = jnp.where(lane_of(first) < 2 * width, first, pltpu.roll(second, width, 1))


def late_gram_kernel(pad, split1, split2, early_ref, out_ref):
    width = out_ref.shape[0]
    (late,) = gram(pad, (split2,), (split1, split2))
    out_ref[...] = jnp.where(lane_of(late) < 3 * width, early_ref[...], pltpu.roll(late, 3 * width, 1))


def places(width, lanes):
    row = lax.broadcasted_iota(jnp.int32, (width, lanes), 0)
    lane = lax.broadcasted_iota(jnp.int32, (width, lanes), 1)
    return row, lane, lane % width


def pack(moments):
    width, lanes = moments.shape
    row, lane, col = places(width, lanes)
    odd = pltpu.roll(moments, lanes - width, 1)
    tiles = jnp.where(row <= col, moments, odd)
    diagonal = jnp.sum(jnp.where(row == col, odd, 0.0), axis=0, keepdims=True)
    half = width // 2
    row, lane = row[:half], lane[:half]
    packed = jnp.where(lane % (2 * width) < width, tiles[:half], pltpu.roll(tiles[half:], width, 1))
    packed = jnp.where(lane < 6 * width, packed, 0.0)
    for k in range(3):
        here = (row == k) & (lane >= 6 * width) & (lane < 7 * width)
        packed = jnp.where(here, pltpu.roll(diagonal, (6 - 2 * k) * width, 1), packed)
    return packed


def unpack(packed):
    half, lanes = packed.shape
    width = 2 * half
    row, lane, col = places(width, lanes)
    tiles = jnp.concatenate([packed, pltpu.roll(packed, lanes - width, 1)], axis=0)
    turned = jnp.concatenate([tiles, jnp.zeros((lanes - width, lanes), F32)], axis=0).T
    mirror = jnp.zeros_like(tiles)
    diagonal = jnp.zeros_like(tiles)
    for k in range(3):
        here = (lane >= 2 * k * width) & (lane < (2 * k + 1) * width)
        part = turned[2 * k * width : (2 * k + 1) * width]
        mirror = jnp.where(here, pltpu.roll(part, 2 * k * width, 1) if k else part, mirror)
        diagonal = jnp.where(here, pltpu.roll(packed[k : k + 1], lanes - (6 - 2 * k) * width, 1), diagonal)
    even = jnp.where(row <= col, tiles, mirror)
    odd = jnp.where(row > col, tiles, jnp.where(row < col, mirror, diagonal))
    both = jnp.where(lane % (2 * width) < width, even, pltpu.roll(odd, width, 1))
    return jnp.where(lane < 6 * width, both, 0.0)


def last_link_kernel(dev_count, pad, rows_ref, base_ref, links_ref, split2, moments_ref, *refs):
    count = len(MATCHINGS)
    far_refs, split_ref, out_ref, field_ref = refs[:count], refs[count], refs[count + 1], refs[-1]
    add_links(dev_count, rows_ref, base_ref, links_ref, far_refs, field_ref)
    split_field(field_ref, split_ref, pad)
    width = moments_ref.shape[0]
    (last,) = gram(pad, (split2,), (split_ref,))
    mine = jnp.where(lane_of(last) < 5 * width, moments_ref[...], pltpu.roll(last, 5 * width, 1))
    mine = pack(mine)
    for peer in range(out_ref.shape[0]):
        out_ref[peer] = mine


def finish_kernel(pad, gathered_ref, split0, split1, split2, split3, solution_ref, residual_ref, doubt_ref):
    peers, half, lanes = gathered_ref.shape
    width = 2 * half
    block_rows = solution_ref.shape[0]
    sums = [gathered_ref[peer] for peer in range(peers)]
    while len(sums) > 1:
        sums = [sum(sums[k + 1 : k + 2], sums[k]) for k in range(0, len(sums), 2)]
    moments = unpack(sums[0])
    table = [pltpu.roll(moments, lanes - width * (k + 1), 1) for k in range(ITERS)] + [moments]
    table = jnp.concatenate(table, axis=0)
    lane = lax.broadcasted_iota(jnp.int32, (1, lanes), 1)
    across = lax.broadcasted_iota(jnp.int32, table.shape, 1) == lax.broadcasted_iota(jnp.int32, table.shape, 0)
    diagonal = jnp.sum(jnp.where(across, table, 0.0), axis=0, keepdims=True)
    pivots = jnp.zeros((1, lanes), F32)
    column = lambda k: jnp.broadcast_to(table[:, k : k + 1], table.shape)
    ahead = {k: (column(k), column(k + 1)) for k in range(0, 2 * AHEAD, 2)}
    for k in range(0, ITERS * width, 2):
        if k and k % 8 == 0:
            table = table[8:]
            ahead = {key: (one[8:], two[8:]) for key, (one, two) in ahead.items()}
        if k + 2 * AHEAD < ITERS * width:
            ahead[k + 2 * AHEAD] = (column(k + 2 * AHEAD), column(k + 2 * AHEAD + 1))
        at = k % 8
        left, right = ahead.pop(k)
        p11, p12 = left[at : at + 1], right[at : at + 1]
        p21, p22 = left[at + 1 : at + 2], right[at + 1 : at + 2]
        det = p11 * p22 - p12 * p21
        inverse = 1.0 / det
        pivots = jnp.where(lane == k, p11, jnp.where(lane == k + 1, det / p11, pivots))
        left, right = (left * p22 - right * p21) * inverse, (right * p11 - left * p12) * inverse
        clear = lambda value: value - left * value[at : at + 1] - right * value[at + 1 : at + 2]
        ahead = {key: (clear(one), clear(two)) for key, (one, two) in ahead.items()}
        table = jnp.where(lane == k, left, jnp.where(lane == k + 1, right, clear(table)))
    trusted = (pivots > TRUSTED_PIVOT * diagonal) & (pivots < jnp.inf)
    used = lane < ITERS * width
    doubt = jnp.where(used & jnp.logical_not(trusted), 1.0, 0.0)
    doubt_ref[0] = jnp.max(doubt).astype(jnp.int32)
    coeffs = table[-width:]
    lane = lax.broadcasted_iota(jnp.int32, coeffs.shape, 1)
    unit = (lane == lax.broadcasted_iota(jnp.int32, coeffs.shape, 0)).astype(F32)
    for_solution = jnp.where(lane < ITERS * width, coeffs, 0.0)
    for_residual = jnp.where(lane < width, unit, jnp.where(lane < LEVELS * width, -pltpu.roll(coeffs, width, 1), 0.0))
    both = jnp.concatenate([for_solution, for_residual], axis=0)
    both = jnp.concatenate([both + pltpu.roll(both, 64, 1), both], axis=1)[:, : PIECES * LEVELS * width]
    left = jnp.concatenate(pieces_of(both), axis=0)
    refs = (split0, split1, split2, split3)
    step = 4

    def body(index, carry):
        cols = pl.ds(pl.multiple_of((pad + index * step) * 128, 128), step * 128)
        right = [ref[piece * width : (piece + 1) * width, cols] for piece in range(PIECES) for ref in refs]
        total = fold(jnp.dot(left, jnp.concatenate(right, axis=0), preferred_element_type=F32), 2 * width)
        for k in range(step):
            solution_ref[index * step + k] = total[:width, k * 128 : (k + 1) * 128]
            residual_ref[index * step + k] = total[width:, k * 128 : (k + 1) * 128]
        return carry

    lax.fori_loop(0, block_rows // step, body, 0, unroll=2)


def gram_matrix(left, right):
    return lax.psum(jnp.einsum("nsi,nti->st", left, right, precision=HIGHEST), "dom")


def mix_columns(field, coeffs):
    return jnp.einsum("nsi,st->nti", field, coeffs, precision=HIGHEST)


def solve_gram(matrix, target):
    factor = jnp.linalg.cholesky(0.5 * (matrix + matrix.T))
    return jax.scipy.linalg.cho_solve((factor, True), target)


def plain_kernel(field_ref, band_ref, out_ref):
    row = pl.program_id(0)
    total = jnp.zeros(out_ref.shape[1:], F32)
    for k in range(band_ref.shape[1]):
        total += lax.dot_general(
            field_ref[row + k], band_ref[0, k], (((1,), (1,)), ((), ())), precision=HIGHEST, preferred_element_type=F32
        )
    out_ref[0] = total


def apply_operator(field, band_blocks, link_blocks, link_rows):
    dev_count = lax.axis_size("dom")
    block_rows, band = band_blocks.shape[:2]
    half = band // 2
    picks = (link_rows[0][:, :, None] == jnp.arange(block_rows, dtype=jnp.int32)).astype(field.dtype)
    padded = jnp.pad(field, ((half, half), (0, 0), (0, 0)))
    total = pl.pallas_call(
        plain_kernel,
        out_shape=jax.ShapeDtypeStruct(field.shape, F32),
        grid=(block_rows,),
        in_specs=[
            pl.BlockSpec(padded.shape, lambda r: (0, 0, 0)),
            pl.BlockSpec((1, *band_blocks.shape[1:]), lambda r: (r, 0, 0, 0)),
        ],
        out_specs=pl.BlockSpec((1, *field.shape[1:]), lambda r: (r, 0, 0)),
        compiler_params=params(8),
        name="plain",
    )(padded, band_blocks)
    for face in range(link_rows.shape[1]):
        by = offsets(dev_count)[face // 2] * (1 - 2 * (face % 2))
        source = jnp.einsum("hr,rsi->hsi", picks[face ^ 1], field, precision=HIGHEST)
        far = lax.ppermute(source, "dom", [(i, (i - by) % dev_count) for i in range(dev_count)])
        part = jnp.einsum("hsj,hij->hsi", far, link_blocks[0, face], precision=HIGHEST)
        total += jnp.einsum("hr,hsi->rsi", picks[face], part, precision=HIGHEST)
    return total


def classical(right_side, band_blocks, link_blocks, link_rows):
    def iterate(_, state):
        value, rest, direction, squares = state
        image = apply_operator(direction, band_blocks, link_blocks, link_rows)
        alpha = solve_gram(gram_matrix(direction, image), squares)
        value = value + mix_columns(direction, alpha)
        rest = rest - mix_columns(image, alpha)
        fresh = gram_matrix(rest, rest)
        direction = rest + mix_columns(direction, solve_gram(squares, fresh))
        return value, rest, direction, fresh

    start = (jnp.zeros_like(right_side), right_side, right_side, gram_matrix(right_side, right_side))
    return lax.fori_loop(0, ITERS, iterate, start)[:2]


def shards(*args):
    right_side, band_blocks, link_blocks, link_rows = args
    dev_count = lax.axis_size("dom")
    block_rows, width, size = right_side.shape
    band = band_blocks.shape[1]
    half = band // 2
    faces, slots = link_rows.shape[1:]
    pairs = block_rows // 2
    count = len(MATCHINGS)
    message = jax.ShapeDtypeStruct((slots, width, size), F32)
    split = jax.ShapeDtypeStruct((PIECES * width, (block_rows + 2 * half) * size), BF16)
    field = jax.ShapeDtypeStruct(right_side.shape, F32)

    def exchange(messages):
        got = []
        for index, (pair, phase) in enumerate(MATCHINGS):
            got.append(lax.ppermute(messages[index], "dom", matching_pairs(dev_count, pair, phase)))
        return got

    hbm = [pl.BlockSpec(memory_space=pltpu.HBM)]
    right_side, band_blocks, link_blocks = (
        pltpu.with_memory_space_constraint(value, pltpu.HBM) for value in (right_side, band_blocks, link_blocks)
    )
    slot_rows = pltpu.with_memory_space_constraint(jnp.swapaxes(link_rows, 1, 2), pltpu.HBM)
    messages = pl.pallas_call(
        functools.partial(first_send_kernel, dev_count),
        out_shape=[message] * count,
        in_specs=hbm * 2,
        out_specs=vmem(count),
        scratch_shapes=[
            pltpu.SMEM(slot_rows.shape, jnp.int32),
            pltpu.VMEM(right_side.shape, F32),
            pltpu.SemaphoreType.DMA((2,)),
        ],
        compiler_params=params(8),
        name="first_send",
    )(slot_rows, right_side)
    far = exchange(messages)
    weights, links, split0, base = pl.pallas_call(
        functools.partial(prepare_kernel, half),
        out_shape=[
            pltpu.VMEM((pairs + 2, 2 * (band + 1), size, 2 * size), BF16),
            pltpu.VMEM((faces, slots // 2, 2 * size, 2 * size), BF16),
            split,
            field,
        ],
        in_specs=hbm * 3,
        out_specs=vmem(4),
        scratch_shapes=[
            pltpu.VMEM(right_side.shape, F32),
            pltpu.VMEM(band_blocks.shape, F32),
            pltpu.VMEM(link_blocks.shape[1:], F32),
            pltpu.VMEM((block_rows + 2 * half, width, size), F32),
            pltpu.SemaphoreType.DMA((pairs + 2,)),
        ],
        compiler_params=params(18),
        cost_estimate=pl.CostEstimate(flops=10**9, bytes_accessed=12 * 10**6, transcendentals=0),
        name="prepare",
    )(right_side, band_blocks, link_blocks)

    splits = [split0]
    moments = None
    for level in range(ITERS):
        if level > 0:
            base, latest = pl.pallas_call(
                functools.partial(band_kernel, half),
                out_shape=[field, split],
                in_specs=vmem(2),
                out_specs=vmem(2),
                compiler_params=params(8),
                cost_estimate=pl.CostEstimate(flops=10**9, bytes_accessed=12 * 10**6, transcendentals=0),
                name="band",
            )(weights, values)
            splits.append(latest)
            late = level == ITERS - 1
            moments = pl.pallas_call(
                functools.partial(late_gram_kernel if late else early_gram_kernel, half),
                out_shape=jax.ShapeDtypeStruct((width, 128), F32),
                in_specs=vmem(2 + late),
                out_specs=vmem(1)[0],
                compiler_params=params(8),
                cost_estimate=pl.CostEstimate(flops=10**9, bytes_accessed=4 * 10**6, transcendentals=0),
                name="gram",
            )(*splits[-2:], *([moments] if late else []))
        if level + 1 < ITERS:
            values, *messages = pl.pallas_call(
                functools.partial(link_kernel, dev_count),
                out_shape=[field] + [message] * count,
                in_specs=[smem()] + vmem(2 + count),
                out_specs=vmem(1 + count),
                compiler_params=params(8),
                name="link",
            )(slot_rows, base, links, *far)
            far = exchange(messages)
    split3, mine = pl.pallas_call(
        functools.partial(last_link_kernel, dev_count, half),
        out_shape=[split, jax.ShapeDtypeStruct((dev_count, width // 2, 128), F32)],
        in_specs=[smem()] + vmem(4 + count),
        out_specs=vmem(2),
        scratch_shapes=[pltpu.VMEM(right_side.shape, F32)],
        compiler_params=params(8),
        name="last_link",
    )(slot_rows, base, links, splits[-1], moments, *far)
    splits.append(split3)
    gathered = lax.all_to_all(mine, "dom", 0, 0)
    value, rest, doubt = pl.pallas_call(
        functools.partial(finish_kernel, half),
        out_shape=[field, field, jax.ShapeDtypeStruct((1,), jnp.int32)],
        in_specs=vmem(1 + LEVELS),
        out_specs=vmem(2) + [smem()],
        compiler_params=params(8),
        name="finish",
    )(gathered, *splits)
    again = lambda state: state[0][0] > 0

    def redo(state):
        held, flag = lax.optimization_barrier((args, state[0]))
        return 0 * flag, *classical(*held)

    return lax.while_loop(again, redo, (doubt, value, rest))[1:]


def solution(mesh):
    in_specs = (
        P("dom", None, None),
        P("dom", None, None, None),
        P("dom", None, None, None, None),
        P("dom", None, None),
    )
    out_specs = (P("dom", None, None), P("dom", None, None))
    return jax.shard_map(
        lambda *args: tuple(shards(*args)), mesh=mesh, in_specs=in_specs, out_specs=out_specs, check_vma=False
    )
```

```python
import functools

import jax
import jax.numpy as jnp
from jax import lax
from jax.experimental import pallas as pl
from jax.experimental.pallas import tpu as pltpu
from jax.sharding import PartitionSpec as P


ITERS = 3
TRUSTED_PIVOT = 0.008
AHEAD = 3
HIGHEST = lax.Precision.HIGHEST
LEVELS = ITERS + 1
PIECES = 3
F32 = jnp.float32
BF16 = jnp.bfloat16
MIB = 1 << 20

MATCHINGS = ((0, 1), (1, 1), (2, 1), (2, 0), (1, 0), (0, 0))


def offsets(dev_count):
    return (1, dev_count // 16, dev_count // 4)


def matching_pairs(dev_count, pair, phase):
    off = offsets(dev_count)[pair]
    return [
        (i, (i + off) % dev_count if (i // off + phase) % 2 == 0 else (i - off) % dev_count)
        for i in range(dev_count)
    ]


def matching_face(dev_count, pair, phase):
    me = lax.axis_index("dom")
    return 2 * pair + lax.rem(me // offsets(dev_count)[pair] + phase, 2)


def pieces_of(value):
    high = value.astype(BF16)
    rest = value - high.astype(F32)
    mid = rest.astype(BF16)
    low = (rest - mid.astype(F32)).astype(BF16)
    return high, mid, low


def vmem(count):
    return [pl.BlockSpec(memory_space=pltpu.VMEM)] * count


def smem():
    return pl.BlockSpec(memory_space=pltpu.SMEM)


def params(mib):
    return pltpu.CompilerParams(vmem_limit_bytes=mib * MIB)


def send_rows(dev_count, rows_ref, field_ref, out_refs):
    block_rows = field_ref.shape[0]
    for (pair, phase), out_ref in zip(MATCHINGS, out_refs):
        face = matching_face(dev_count, pair, phase)
        for slot in range(rows_ref.shape[1]):
            row = jnp.minimum(rows_ref[0, slot, face], block_rows - 1)
            out_ref[slot] = field_ref[row]


def split_field(field_ref, split_ref, pad):
    block_rows, width, size = field_ref.shape
    zero = jnp.zeros((split_ref.shape[0], pad * size), BF16)
    split_ref[:, : pad * size] = zero
    split_ref[:, (pad + block_rows) * size :] = zero
    for row in range(block_rows):
        cols = slice((pad + row) * size, (pad + row + 1) * size)
        for piece, value in enumerate(pieces_of(field_ref[row])):
            split_ref[piece * width : (piece + 1) * width, cols] = value


def first_send_kernel(dev_count, rows_hbm, field_hbm, *refs):
    out_refs, (rows_ref, field_ref, sems) = refs[:-3], refs[-3:]
    fetch_field = pltpu.make_async_copy(field_hbm, field_ref, sems.at[0])
    fetch_rows = pltpu.make_async_copy(rows_hbm, rows_ref, sems.at[1])
    fetch_field.start()
    fetch_rows.start()
    fetch_rows.wait()
    fetch_field.wait()
    send_rows(dev_count, rows_ref, field_ref, out_refs)


def fold(value, width):
    total = value[(PIECES - 1) * width : PIECES * width]
    for piece in range(PIECES - 2, -1, -1):
        total = total + value[piece * width : (piece + 1) * width]
    return total


def pair_product(weights_ref, split_ref, out_ref, pair):
    _, width, size = out_ref.shape
    depth = weights_ref.shape[1] * size
    start = pl.multiple_of(pair * 2 * size, 2 * size)
    rows = split_ref[:, pl.ds(start, depth // 2)]
    both = jnp.concatenate([rows, rows], axis=1)
    weights = weights_ref[pair + 1].reshape(depth, 2 * size)
    total = fold(jnp.dot(both, weights, preferred_element_type=F32), width)
    out_ref[2 * pair] = total[:, :size]
    out_ref[2 * pair + 1] = total[:, size:]


def band_kernel(pad, weights_ref, field_ref, out_ref, split_ref):
    split_field(field_ref, split_ref, pad)

    def body(pair, carry):
        pair_product(weights_ref, split_ref, out_ref, pair)
        return carry

    lax.fori_loop(0, out_ref.shape[0] // 2, body, 0, unroll=True)


def prepare_kernel(
    half, field_hbm, band_hbm, link_hbm, weights_ref, links_ref, split_ref, out_ref, field_ref, band_ref, link_ref, total_ref, sems
):
    block_rows, band, size, _ = band_ref.shape
    faces, count = link_ref.shape[:2]
    pairs = block_rows // 2
    span = band + 1
    copies = [pltpu.make_async_copy(field_hbm, field_ref, sems.at[pairs])]
    copies += [
        pltpu.make_async_copy(band_hbm.at[pl.ds(2 * pair, 2)], band_ref.at[pl.ds(2 * pair, 2)], sems.at[pair])
        for pair in range(pairs)
    ]
    copies.append(pltpu.make_async_copy(link_hbm.at[0], link_ref, sems.at[pairs + 1]))
    for copy in copies:
        copy.start()
    wide = jnp.zeros((size, 2 * size), BF16)
    for copy in range(2):
        for place in range(half):
            weights_ref[1, copy * span + place] = wide
            weights_ref[pairs, copy * span + span - 1 - place] = wide
        for pair in range(1, pairs + 1):
            weights_ref[pair, copy * span, :, size:] = wide[:, :size]
            weights_ref[pair, copy * span + span - 1, :, :size] = wide[:, :size]
    total_ref[...] = jnp.zeros_like(total_ref)
    copies[0].wait()
    split_field(field_ref, split_ref, half)

    def convert(step, carry):
        here = pl.ds(2 * step, 2)
        pltpu.make_async_copy(band_hbm.at[here], band_ref.at[here], sems.at[step]).wait()
        for even in range(2):
            rows = split_ref[:, pl.ds(pl.multiple_of((half + 2 * step + even) * size, size), size)]
            both = jnp.concatenate([rows, rows], axis=1)
            for k in range(band):
                shift = (even + k - half) // 2
                col = (even + k - half) % 2
                place = even + half - 2 * shift
                block = band_ref[2 * step + even, k]
                high = block.astype(BF16)
                low = (block - high.astype(F32)).astype(BF16)
                cols = slice(col * size, (col + 1) * size)
                weights_ref[step + shift + 1, place, :, cols] = high
                weights_ref[step + shift + 1, span + place, :, cols] = low
                product = jnp.dot(both, jnp.concatenate([high, low], axis=0), preferred_element_type=F32)
                total_ref[2 * step + even + k] += fold(product, field_ref.shape[1])
        return carry

    lax.fori_loop(0, pairs, convert, 0)
    out_ref[...] = total_ref[pl.ds(half, block_rows)]
    copies[-1].wait()

    def convert_links(face, carry):
        for slot in range(count):
            block = link_ref[face, slot].T
            high = block.astype(BF16)
            low = (block - high.astype(F32)).astype(BF16)
            cols = slice(slot % 2 * size, (slot % 2 + 1) * size)
            links_ref[face, slot // 2, :size, cols] = high
            links_ref[face, slot // 2, size:, cols] = low
        return carry

    lax.fori_loop(0, faces, convert_links, 0, unroll=True)


def add_links(dev_count, rows_ref, base_ref, links_ref, far_refs, field_ref):
    block_rows, width, size = base_ref.shape
    field_ref[...] = base_ref[...]
    for (pair, phase), far_ref in zip(MATCHINGS, far_refs):
        face = matching_face(dev_count, pair, phase)
        for two in range(far_ref.shape[0] // 2):
            stacked = []
            for slot in (2 * two, 2 * two + 1):
                stacked.extend(pieces_of(far_ref[slot]))
            rows = jnp.concatenate(stacked, axis=0)
            both = jnp.concatenate([rows, rows], axis=1)
            product = jnp.dot(both, links_ref[face, two], preferred_element_type=F32)
            for k in range(2):
                part = product[k * PIECES * width : (k + 1) * PIECES * width, k * size : (k + 1) * size]
                row = jnp.minimum(rows_ref[0, 2 * two + k, face], block_rows - 1)
                field_ref[row] = field_ref[row] + fold(part, width)


def link_kernel(dev_count, rows_ref, base_ref, links_ref, *refs):
    count = len(MATCHINGS)
    far_refs, field_ref, out_refs = refs[:count], refs[count], refs[count + 1 :]
    add_links(dev_count, rows_ref, base_ref, links_ref, far_refs, field_ref)
    send_rows(dev_count, rows_ref, field_ref, out_refs)


def gram(pad, left_refs, right_refs):
    rows, lanes = left_refs[0].shape
    width = rows // PIECES
    cols = slice(pad * 128, lanes - pad * 128)
    left = jnp.concatenate([ref[:, cols] for ref in left_refs], axis=0)
    right = [ref[piece * width : (piece + 1) * width, cols] for piece in range(PIECES) for ref in right_refs]
    right += [jnp.zeros_like(right[0])] * (128 // width - len(right))
    dims = (((1,), (1,)), ((), ()))
    product = lax.dot_general(left, jnp.concatenate(right, axis=0), dims, preferred_element_type=F32)
    step = len(right_refs) * width
    sums = []
    for k in range(len(left_refs)):
        part = fold(product[rows * k : rows * (k + 1)], width)
        total = part
        for piece in range(1, PIECES):
            total = total + pltpu.roll(part, 128 - piece * step, 1)
        sums.append(total)
    return sums


def lane_of(value):
    return lax.broadcasted_iota(jnp.int32, value.shape, 1)


def early_gram_kernel(pad, split0, split1, out_ref):
    width = out_ref.shape[0]
    first, second = gram(pad, (split0, split1), (split0, split1))
    out_ref[...] = jnp.where(lane_of(first) < 2 * width, first, pltpu.roll(second, width, 1))


def late_gram_kernel(pad, split1, split2, early_ref, out_ref):
    width = out_ref.shape[0]
    (late,) = gram(pad, (split2,), (split1, split2))
    out_ref[...] = jnp.where(lane_of(late) < 3 * width, early_ref[...], pltpu.roll(late, 3 * width, 1))


def places(width, lanes):
    row = lax.broadcasted_iota(jnp.int32, (width, lanes), 0)
    lane = lax.broadcasted_iota(jnp.int32, (width, lanes), 1)
    return row, lane, lane % width


def pack(moments):
    width, lanes = moments.shape
    row, lane, col = places(width, lanes)
    odd = pltpu.roll(moments, lanes - width, 1)
    tiles = jnp.where(row <= col, moments, odd)
    diagonal = jnp.sum(jnp.where(row == col, odd, 0.0), axis=0, keepdims=True)
    half = width // 2
    row, lane = row[:half], lane[:half]
    packed = jnp.where(lane % (2 * width) < width, tiles[:half], pltpu.roll(tiles[half:], width, 1))
    packed = jnp.where(lane < 6 * width, packed, 0.0)
    for k in range(3):
        here = (row == k) & (lane >= 6 * width) & (lane < 7 * width)
        packed = jnp.where(here, pltpu.roll(diagonal, (6 - 2 * k) * width, 1), packed)
    return packed


def unpack(packed):
    half, lanes = packed.shape
    width = 2 * half
    row, lane, col = places(width, lanes)
    tiles = jnp.concatenate([packed, pltpu.roll(packed, lanes - width, 1)], axis=0)
    turned = jnp.concatenate([tiles, jnp.zeros((lanes - width, lanes), F32)], axis=0).T
    mirror = jnp.zeros_like(tiles)
    diagonal = jnp.zeros_like(tiles)
    for k in range(3):
        here = (lane >= 2 * k * width) & (lane < (2 * k + 1) * width)
        part = turned[2 * k * width : (2 * k + 1) * width]
        mirror = jnp.where(here, pltpu.roll(part, 2 * k * width, 1) if k else part, mirror)
        diagonal = jnp.where(here, pltpu.roll(packed[k : k + 1], lanes - (6 - 2 * k) * width, 1), diagonal)
    even = jnp.where(row <= col, tiles, mirror)
    odd = jnp.where(row > col, tiles, jnp.where(row < col, mirror, diagonal))
    both = jnp.where(lane % (2 * width) < width, even, pltpu.roll(odd, width, 1))
    return jnp.where(lane < 6 * width, both, 0.0)


def last_link_kernel(dev_count, pad, rows_ref, base_ref, links_ref, split2, moments_ref, *refs):
    count = len(MATCHINGS)
    far_refs, split_ref, out_ref, field_ref = refs[:count], refs[count], refs[count + 1], refs[-1]
    add_links(dev_count, rows_ref, base_ref, links_ref, far_refs, field_ref)
    split_field(field_ref, split_ref, pad)
    width = moments_ref.shape[0]
    (last,) = gram(pad, (split2,), (split_ref,))
    mine = jnp.where(lane_of(last) < 5 * width, moments_ref[...], pltpu.roll(last, 5 * width, 1))
    mine = pack(mine)
    for peer in range(out_ref.shape[0]):
        out_ref[peer] = mine


def finish_kernel(pad, gathered_ref, split0, split1, split2, split3, solution_ref, residual_ref, doubt_ref):
    peers, half, lanes = gathered_ref.shape
    width = 2 * half
    block_rows = solution_ref.shape[0]
    sums = [gathered_ref[peer] for peer in range(peers)]
    while len(sums) > 1:
        sums = [sum(sums[k + 1 : k + 2], sums[k]) for k in range(0, len(sums), 2)]
    moments = unpack(sums[0])
    table = [pltpu.roll(moments, lanes - width * (k + 1), 1) for k in range(ITERS)] + [moments]
    table = jnp.concatenate(table, axis=0)
    lane = lax.broadcasted_iota(jnp.int32, (1, lanes), 1)
    across = lax.broadcasted_iota(jnp.int32, table.shape, 1) == lax.broadcasted_iota(jnp.int32, table.shape, 0)
    diagonal = jnp.sum(jnp.where(across, table, 0.0), axis=0, keepdims=True)
    pivots = jnp.zeros((1, lanes), F32)
    column = lambda k: jnp.broadcast_to(table[:, k : k + 1], table.shape)
    ahead = {k: (column(k), column(k + 1)) for k in range(0, 2 * AHEAD, 2)}
    for k in range(0, ITERS * width, 2):
        if k and k % 8 == 0:
            table = table[8:]
            ahead = {key: (one[8:], two[8:]) for key, (one, two) in ahead.items()}
        if k + 2 * AHEAD < ITERS * width:
            ahead[k + 2 * AHEAD] = (column(k + 2 * AHEAD), column(k + 2 * AHEAD + 1))
        at = k % 8
        left, right = ahead.pop(k)
        p11, p12 = left[at : at + 1], right[at : at + 1]
        p21, p22 = left[at + 1 : at + 2], right[at + 1 : at + 2]
        det = p11 * p22 - p12 * p21
        inverse = 1.0 / det
        pivots = jnp.where(lane == k, p11, jnp.where(lane == k + 1, det / p11, pivots))
        left, right = (left * p22 - right * p21) * inverse, (right * p11 - left * p12) * inverse
        clear = lambda value: value - left * value[at : at + 1] - right * value[at + 1 : at + 2]
        ahead = {key: (clear(one), clear(two)) for key, (one, two) in ahead.items()}
        table = jnp.where(lane == k, left, jnp.where(lane == k + 1, right, clear(table)))
    trusted = (pivots > TRUSTED_PIVOT * diagonal) & (pivots < jnp.inf)
    used = lane < ITERS * width
    doubt = jnp.where(used & jnp.logical_not(trusted), 1.0, 0.0)
    doubt_ref[0] = jnp.max(doubt).astype(jnp.int32)
    coeffs = table[-width:]
    lane = lax.broadcasted_iota(jnp.int32, coeffs.shape, 1)
    unit = (lane == lax.broadcasted_iota(jnp.int32, coeffs.shape, 0)).astype(F32)
    for_solution = jnp.where(lane < ITERS * width, coeffs, 0.0)
    for_residual = jnp.where(lane < width, unit, jnp.where(lane < LEVELS * width, -pltpu.roll(coeffs, width, 1), 0.0))
    both = jnp.concatenate([for_solution, for_residual], axis=0)
    both = jnp.concatenate([both + pltpu.roll(both, 64, 1), both], axis=1)[:, : PIECES * LEVELS * width]
    left = jnp.concatenate(pieces_of(both), axis=0)
    refs = (split0, split1, split2, split3)
    step = 4

    def body(index, carry):
        cols = pl.ds(pl.multiple_of((pad + index * step) * 128, 128), step * 128)
        right = [ref[piece * width : (piece + 1) * width, cols] for piece in range(PIECES) for ref in refs]
        total = fold(jnp.dot(left, jnp.concatenate(right, axis=0), preferred_element_type=F32), 2 * width)
        for k in range(step):
            solution_ref[index * step + k] = total[:width, k * 128 : (k + 1) * 128]
            residual_ref[index * step + k] = total[width:, k * 128 : (k + 1) * 128]
        return carry

    lax.fori_loop(0, block_rows // step, body, 0, unroll=True)


def gram_matrix(left, right):
    return lax.psum(jnp.einsum("nsi,nti->st", left, right, precision=HIGHEST), "dom")


def mix_columns(field, coeffs):
    return jnp.einsum("nsi,st->nti", field, coeffs, precision=HIGHEST)


def solve_gram(matrix, target):
    factor = jnp.linalg.cholesky(0.5 * (matrix + matrix.T))
    return jax.scipy.linalg.cho_solve((factor, True), target)


def plain_kernel(field_ref, band_ref, out_ref):
    row = pl.program_id(0)
    total = jnp.zeros(out_ref.shape[1:], F32)
    for k in range(band_ref.shape[1]):
        total += lax.dot_general(
            field_ref[row + k], band_ref[0, k], (((1,), (1,)), ((), ())), precision=HIGHEST, preferred_element_type=F32
        )
    out_ref[0] = total


def apply_operator(field, band_blocks, link_blocks, link_rows):
    dev_count = lax.axis_size("dom")
    block_rows, band = band_blocks.shape[:2]
    half = band // 2
    picks = (link_rows[0][:, :, None] == jnp.arange(block_rows, dtype=jnp.int32)).astype(field.dtype)
    padded = jnp.pad(field, ((half, half), (0, 0), (0, 0)))
    total = pl.pallas_call(
        plain_kernel,
        out_shape=jax.ShapeDtypeStruct(field.shape, F32),
        grid=(block_rows,),
        in_specs=[
            pl.BlockSpec(padded.shape, lambda r: (0, 0, 0)),
            pl.BlockSpec((1, *band_blocks.shape[1:]), lambda r: (r, 0, 0, 0)),
        ],
        out_specs=pl.BlockSpec((1, *field.shape[1:]), lambda r: (r, 0, 0)),
        compiler_params=params(8),
        name="plain",
    )(padded, band_blocks)
    for face in range(link_rows.shape[1]):
        by = offsets(dev_count)[face // 2] * (1 - 2 * (face % 2))
        source = jnp.einsum("hr,rsi->hsi", picks[face ^ 1], field, precision=HIGHEST)
        far = lax.ppermute(source, "dom", [(i, (i - by) % dev_count) for i in range(dev_count)])
        part = jnp.einsum("hsj,hij->hsi", far, link_blocks[0, face], precision=HIGHEST)
        total += jnp.einsum("hr,hsi->rsi", picks[face], part, precision=HIGHEST)
    return total


def classical(right_side, band_blocks, link_blocks, link_rows):
    def iterate(_, state):
        value, rest, direction, squares = state
        image = apply_operator(direction, band_blocks, link_blocks, link_rows)
        alpha = solve_gram(gram_matrix(direction, image), squares)
        value = value + mix_columns(direction, alpha)
        rest = rest - mix_columns(image, alpha)
        fresh = gram_matrix(rest, rest)
        direction = rest + mix_columns(direction, solve_gram(squares, fresh))
        return value, rest, direction, fresh

    start = (jnp.zeros_like(right_side), right_side, right_side, gram_matrix(right_side, right_side))
    return lax.fori_loop(0, ITERS, iterate, start)[:2]


def shards(*args):
    right_side, band_blocks, link_blocks, link_rows = args
    dev_count = lax.axis_size("dom")
    block_rows, width, size = right_side.shape
    band = band_blocks.shape[1]
    half = band // 2
    faces, slots = link_rows.shape[1:]
    pairs = block_rows // 2
    count = len(MATCHINGS)
    message = jax.ShapeDtypeStruct((slots, width, size), F32)
    split = jax.ShapeDtypeStruct((PIECES * width, (block_rows + 2 * half) * size), BF16)
    field = jax.ShapeDtypeStruct(right_side.shape, F32)

    def exchange(messages):
        got = []
        for index, (pair, phase) in enumerate(MATCHINGS):
            got.append(lax.ppermute(messages[index], "dom", matching_pairs(dev_count, pair, phase)))
        return got

    hbm = [pl.BlockSpec(memory_space=pltpu.HBM)]
    right_side, band_blocks, link_blocks = (
        pltpu.with_memory_space_constraint(value, pltpu.HBM) for value in (right_side, band_blocks, link_blocks)
    )
    slot_rows = pltpu.with_memory_space_constraint(jnp.swapaxes(link_rows, 1, 2), pltpu.HBM)
    messages = pl.pallas_call(
        functools.partial(first_send_kernel, dev_count),
        out_shape=[message] * count,
        in_specs=hbm * 2,
        out_specs=vmem(count),
        scratch_shapes=[
            pltpu.SMEM(slot_rows.shape, jnp.int32),
            pltpu.VMEM(right_side.shape, F32),
            pltpu.SemaphoreType.DMA((2,)),
        ],
        compiler_params=params(8),
        name="first_send",
    )(slot_rows, right_side)
    far = exchange(messages)
    weights, links, split0, base = pl.pallas_call(
        functools.partial(prepare_kernel, half),
        out_shape=[
            pltpu.VMEM((pairs + 2, 2 * (band + 1), size, 2 * size), BF16),
            pltpu.VMEM((faces, slots // 2, 2 * size, 2 * size), BF16),
            split,
            field,
        ],
        in_specs=hbm * 3,
        out_specs=vmem(4),
        scratch_shapes=[
            pltpu.VMEM(right_side.shape, F32),
            pltpu.VMEM(band_blocks.shape, F32),
            pltpu.VMEM(link_blocks.shape[1:], F32),
            pltpu.VMEM((block_rows + 2 * half, width, size), F32),
            pltpu.SemaphoreType.DMA((pairs + 2,)),
        ],
        compiler_params=params(18),
        cost_estimate=pl.CostEstimate(flops=10**9, bytes_accessed=12 * 10**6, transcendentals=0),
        name="prepare",
    )(right_side, band_blocks, link_blocks)

    splits = [split0]
    moments = None
    for level in range(ITERS):
        if level > 0:
            base, latest = pl.pallas_call(
                functools.partial(band_kernel, half),
                out_shape=[field, split],
                in_specs=vmem(2),
                out_specs=vmem(2),
                compiler_params=params(8),
                cost_estimate=pl.CostEstimate(flops=10**9, bytes_accessed=12 * 10**6, transcendentals=0),
                name="band",
            )(weights, values)
            splits.append(latest)
            late = level == ITERS - 1
            moments = pl.pallas_call(
                functools.partial(late_gram_kernel if late else early_gram_kernel, half),
                out_shape=jax.ShapeDtypeStruct((width, 128), F32),
                in_specs=vmem(2 + late),
                out_specs=vmem(1)[0],
                compiler_params=params(8),
                cost_estimate=pl.CostEstimate(flops=10**9, bytes_accessed=4 * 10**6, transcendentals=0),
                name="gram",
            )(*splits[-2:], *([moments] if late else []))
        if level + 1 < ITERS:
            values, *messages = pl.pallas_call(
                functools.partial(link_kernel, dev_count),
                out_shape=[field] + [message] * count,
                in_specs=[smem()] + vmem(2 + count),
                out_specs=vmem(1 + count),
                compiler_params=params(8),
                name="link",
            )(slot_rows, base, links, *far)
            far = exchange(messages)
    split3, mine = pl.pallas_call(
        functools.partial(last_link_kernel, dev_count, half),
        out_shape=[split, jax.ShapeDtypeStruct((dev_count, width // 2, 128), F32)],
        in_specs=[smem()] + vmem(4 + count),
        out_specs=vmem(2),
        scratch_shapes=[pltpu.VMEM(right_side.shape, F32)],
        compiler_params=params(8),
        name="last_link",
    )(slot_rows, base, links, splits[-1], moments, *far)
    splits.append(split3)
    gathered = lax.all_to_all(mine, "dom", 0, 0)
    value, rest, doubt = pl.pallas_call(
        functools.partial(finish_kernel, half),
        out_shape=[field, field, jax.ShapeDtypeStruct((1,), jnp.int32)],
        in_specs=vmem(1 + LEVELS),
        out_specs=vmem(2) + [smem()],
        compiler_params=params(8),
        name="finish",
    )(gathered, *splits)
    again = lambda state: state[0][0] > 0

    def redo(state):
        held, flag = lax.optimization_barrier((args, state[0]))
        return 0 * flag, *classical(*held)

    return lax.while_loop(again, redo, (doubt, value, rest))[1:]


def solution(mesh):
    in_specs = (
        P("dom", None, None),
        P("dom", None, None, None),
        P("dom", None, None, None, None),
        P("dom", None, None),
    )
    out_specs = (P("dom", None, None), P("dom", None, None))
    return jax.shard_map(
        lambda *args: tuple(shards(*args)), mesh=mesh, in_specs=in_specs, out_specs=out_specs, check_vma=False
    )
```
